256 devices in a mesh: dp: 32 (over z_hi, x, y), tensor: 8 (over z_lo, core).
Axes of the slice: x: 4, y: 4, z: 8 (z_hi: 2, z_lo: 4; z = z_hi * 4 + z_lo), core: 2. Of those that a mesh axis runs over, the one named last changes fastest.
Arguments:
- tokens: bfloat16 [8192, 4096], P(('dp', 'tensor')), may hold values from -6 to 6
- out_grad: bfloat16 [8192, 4096], P(('dp', 'tensor')), may hold values from -6 to 6
- weight_tiles: bfloat16 [128, 3, 112, 3, 128], P('dp', None, 'tensor'), may hold values from -0.3125 to 0.3125
- tile_counts: int32 [3, 112], P(None, 'tensor'), may hold values from 1 to 3, as said below
- tile_rows: int32 [3, 112, 3], P(None, 'tensor'), may hold values from 0 to 31, as said below
Outputs:
- ffn_out: bfloat16 [8192, 4096], P(('dp', 'tensor'))
- input_grad: bfloat16 [8192, 4096], P(('dp', 'tensor'))
- tile_grad: bfloat16 [128, 3, 112, 3, 128], P('dp', None, 'tensor')
The draws below stay inside these ranges and needn't reach their ends.
Inputs may be any that keep to these rules, and one draw needn't show every extreme that they name: `tile_counts`: for each matrix and each q, the live slots of hidden blocks q * 14 to (q + 1) * 14 - 1 number at most 28 together, and for each matrix some q reaches 28. `tile_rows`: within one hidden block of one matrix the 3 feature blocks are distinct.
All inputs are finite; a program needn't handle non-finite values.
Results may differ from the reference program's by a relative error of at most 0.018.
Values may be sent and summed in bfloat16 or wider, within the bound.
A program may use at most 128 MiB of HBM per device.

```python
import math
import jax
import jax.numpy as jnp
from jax import lax

D = 4096
TILE = 128
KMAX = 3
DB = 32
FB = 112
FB_DEV = 14
GROUP_ROWS = 256
TOKENS = 8192
N_DP = 32


def draw_tile_counts(key, part):

    def count_row(matrix_key):
        base_key, pick_key = jax.random.split(matrix_key)
        base_count = jax.random.randint(base_key, (FB,), 1, KMAX, dtype=jnp.int32)
        busiest = jax.random.randint(pick_key, (), 0, FB // FB_DEV, dtype=jnp.int32)
        block_ids = jnp.arange(FB, dtype=jnp.int32)
        busy_count = jnp.where(block_ids % 2 == 0, KMAX, KMAX - 2).astype(jnp.int32)
        return jnp.where(block_ids // FB_DEV == busiest, busy_count, base_count).astype(jnp.int32)
    return jnp.stack([count_row(jax.random.fold_in(key, 11 + matrix)) for matrix in range(3)])


def draw_tile_rows(key, part):
    key_list = jax.random.split(jax.random.fold_in(key, 29), 3 * FB)
    picked = jax.vmap(lambda one_key: jax.random.permutation(one_key, DB)[:KMAX])(key_list)
    return picked.reshape(3, FB, KMAX).astype(jnp.int32)


def level_of(key, dims, cuts, low, top_value):
    def one(axis_at, parts):
        heights = jax.random.uniform(jax.random.fold_in(jax.random.fold_in(key, 6), axis_at), (parts,), jnp.float32, low / len(cuts), top_value / len(cuts))
        return jnp.repeat(jnp.exp(heights), dims[axis_at] // parts).reshape((-1,) + (1,) * (len(dims) - axis_at - 1))

    factor_of = one(*cuts[0])
    for cut in cuts[1:]:
        factor_of = factor_of * one(*cut)
    return factor_of


def gaussian(rng, extent, scale, reach, cuts=(), kind=jnp.bfloat16):
    entries = jax.random.normal(rng, extent, jnp.float32) * scale
    if len(cuts) > 0:
        entries = level_of(rng, extent, cuts, -0.22, 0.18) * entries
    return jnp.clip(entries, min=-reach, max=reach).astype(kind)


def setup_inputs(seed: int = 0) -> dict:
    seeds = jax.random.split(jax.random.key(seed), 6)
    tokens = gaussian(seeds[0], (TOKENS, D), 1.0, 6.0, ((0, 256),))
    out_grad = gaussian(seeds[1], (TOKENS, D), 1.0, 6.0, ((0, 256),))
    weight_tiles = gaussian(seeds[2], (TILE, 3, FB, KMAX, TILE), (KMAX * TILE) ** -0.5, 0.3125, ((0, 32), (2, 8)))
    tile_counts = draw_tile_counts(jax.random.fold_in(seeds[5], 71), 0)
    tile_rows = draw_tile_rows(jax.random.fold_in(seeds[5], 71), 0)
    return dict(tokens=tokens, out_grad=out_grad, weight_tiles=weight_tiles, tile_counts=tile_counts, tile_rows=tile_rows)


def reference(tokens, out_grad, weight_tiles, tile_counts, tile_rows):
    highest = lax.Precision.HIGHEST
    slot_total = FB * KMAX
    tile_values = weight_tiles.reshape(TILE, 3, slot_total, TILE).astype(jnp.float32)
    live_mask = (jnp.arange(KMAX, dtype=jnp.int32)[None, None, :] < tile_counts[:, :, None]).astype(jnp.float32).reshape(3, slot_total)
    row_ids = tile_rows.reshape(3, slot_total).astype(jnp.int32)
    row_onehot = (row_ids[:, :, None] == jnp.arange(DB, dtype=jnp.int32)[None, None, :]).astype(jnp.float32) * live_mask[:, :, None]
    grad_scale = 1.0 / math.sqrt(TOKENS)

    def to_blocks(products, matrix):
        masked = products * live_mask[matrix][None, :, None]
        return lax.optimization_barrier(jnp.sum(masked.reshape(GROUP_ROWS, FB, KMAX, TILE), axis=2))

    def from_blocks(values):
        return jnp.repeat(values.astype(jnp.float32), KMAX, axis=1)

    def to_rows(products, matrix):
        return jnp.einsum('tsb,sr->trb', products, row_onehot[matrix], precision=highest)

    def group(running, group_data):
        input_rows, grad_rows = group_data
        input_blocks = input_rows.astype(jnp.float32).reshape(GROUP_ROWS, DB, TILE)
        grad_blocks = grad_rows.astype(jnp.float32).reshape(GROUP_ROWS, DB, TILE)
        gate_sel = jnp.take(input_blocks, row_ids[0], axis=1)
        up_sel = jnp.take(input_blocks, row_ids[1], axis=1)
        gate_pre = to_blocks(jnp.einsum('tsa,asb->tsb', gate_sel, tile_values[:, 0], precision=highest), 0)
        up_pre = to_blocks(jnp.einsum('tsa,asb->tsb', up_sel, tile_values[:, 1], precision=highest), 1)
        gate_sig = jax.nn.sigmoid(gate_pre)
        gate_act = gate_pre * gate_sig
        hidden = (gate_act * up_pre).astype(jnp.bfloat16)
        hidden_sel = from_blocks(hidden)
        ffn_rows = to_rows(jnp.einsum('tsa,asb->tsb', hidden_sel, tile_values[:, 2], precision=highest), 2)
        grad_sel = jnp.take(grad_blocks, row_ids[2], axis=1)
        dh_blocks = to_blocks(jnp.einsum('tsb,asb->tsa', grad_sel, tile_values[:, 2], precision=highest), 2)
        grad_gate = (dh_blocks * up_pre * gate_sig * (1.0 + gate_pre * (1.0 - gate_sig))).astype(jnp.bfloat16)
        grad_up = (dh_blocks * gate_act).astype(jnp.bfloat16)
        dgate_sel = from_blocks(grad_gate)
        dup_sel = from_blocks(grad_up)
        from_gate = to_rows(jnp.einsum('tsb,asb->tsa', dgate_sel, tile_values[:, 0], precision=highest), 0)
        from_up = to_rows(jnp.einsum('tsb,asb->tsa', dup_sel, tile_values[:, 1], precision=highest), 1)
        input_rows_grad = from_gate + from_up
        tile_terms = jnp.stack([jnp.einsum('tsa,tsb->asb', gate_sel, dgate_sel, precision=highest), jnp.einsum('tsa,tsb->asb', up_sel, dup_sel, precision=highest), jnp.einsum('tsa,tsb->asb', hidden_sel, grad_sel, precision=highest)], axis=1)
        tile_terms = tile_terms * (live_mask * grad_scale)[None, :, :, None]
        rounded = lax.optimization_barrier(tile_terms.astype(jnp.bfloat16))
        running = running + rounded.astype(jnp.float32)
        return (running, (ffn_rows.reshape(GROUP_ROWS, D).astype(jnp.bfloat16), input_rows_grad.reshape(GROUP_ROWS, D).astype(jnp.bfloat16)))
    start_sum = jnp.zeros((TILE, 3, slot_total, TILE), jnp.float32)
    group_inputs = (tokens.reshape(N_DP, GROUP_ROWS, D), out_grad.reshape(N_DP, GROUP_ROWS, D))
    total, (ffn_all, input_all) = lax.scan(group, start_sum, group_inputs)
    tile_grad = total.astype(jnp.bfloat16).reshape(TILE, 3, FB, KMAX, TILE)
    return (ffn_all.reshape(TOKENS, D), input_all.reshape(TOKENS, D), tile_grad)
```

```python
import functools
import math

import jax
import jax.numpy as jnp
from jax import lax
from jax.experimental import pallas as pl
from jax.experimental.pallas import tpu as pltpu
from jax.sharding import PartitionSpec as P

MESH = pl.DeviceIdType.MESH
BF = jnp.bfloat16
F32 = jnp.float32
ANY = pl.BlockSpec(memory_space=pl.ANY)
VM = pl.BlockSpec(memory_space=pltpu.VMEM)
SM = pl.BlockSpec(memory_space=pltpu.SMEM)

CAP = 28
SLOTS = 3 * CAP
HALF = SLOTS // 2
BLOCKS = 14
ROWS = 32
WIDTH = 4096
TILE = 128


def places():
    d = lax.axis_index("dp")
    t = lax.axis_index("tensor")
    return d // 16, (d // 4) % 4, d % 4, t // 2, t % 2


def piece_at(zh, x, y):
    return zh * 16 + x * 4 + y


def greet(zh, x, y, z, c):
    barrier = pltpu.get_barrier_semaphore()
    peers = [
        {"tensor": ((z + 1) % 4) * 2 + c},
        {"tensor": ((z + 3) % 4) * 2 + c},
        {"tensor": z * 2 + 1 - c},
        {"dp": piece_at(zh, x, (y + 1) % 4)},
        {"dp": piece_at(zh, x, (y + 3) % 4)},
        {"dp": piece_at(zh, (x + 1) % 4, y)},
        {"dp": piece_at(zh, (x + 3) % 4, y)},
        {"dp": piece_at(1 - zh, x, y)},
    ]
    for peer in peers:
        pl.semaphore_signal(barrier, inc=1, device_id=peer, device_id_type=MESH)
    pl.semaphore_wait(barrier, len(peers))


def gather_kernel(
    counts, x_in, g_in, w_in, x_out, g_out, w_out, w_own, xs_send, xs_recv, w_send, w_recv, local
):
    zh, x, y, z, c = places()
    t = z * 2 + c
    ins, outs = (x_in, g_in), (x_out, g_out)
    greet(zh, x, y, z, c)

    def rows_of(arr, shard):
        return outs[arr].at[pl.ds(pl.multiple_of(shard * ROWS, ROWS), ROWS)]

    def act_copy(arr, shard, way, src, peer):
        return pltpu.make_async_remote_copy(
            src_ref=src,
            dst_ref=rows_of(arr, shard),
            send_sem=xs_send.at[arr, shard, way],
            recv_sem=xs_recv.at[arr, shard],
            device_id={"tensor": peer},
            device_id_type=MESH,
        )

    right, left, mate = t + 2, t - 2, z * 2 + 1 - c

    def to(arr, shard, way, src):
        return act_copy(arr, shard, way, src, (right, left, mate)[way])

    def compact(m):
        def step(i, carry):
            j, k = carry
            w_own[m * CAP + i] = w_in[m * 42 + j * 3 + k]
            more = k + 1 < counts[m, j]
            return (
                jnp.where(more, j, jnp.minimum(j + 1, BLOCKS - 1)),
                jnp.where(more, k + 1, 0),
            )

        lax.fori_loop(0, CAP, step, (jnp.int32(0), jnp.int32(0)))

    for m in range(3):
        compact(m)

    me = piece_at(zh, x, y)
    halves = (pl.ds(0, HALF), pl.ds(HALF, HALF))

    def w_part(piece, half):
        if half is None:
            return w_out.at[:, piece]
        return w_out.at[halves[half], piece]

    def w_copy(piece, half, way, peer, src=None):
        return pltpu.make_async_remote_copy(
            src_ref=w_part(piece, half) if src is None else src,
            dst_ref=w_part(piece, half),
            send_sem=w_send.at[piece, way],
            recv_sem=w_recv.at[piece, 1 if half == 1 else 0],
            device_id={"dp": peer},
            device_id_type=MESH,
        )

    xp, xm = piece_at(zh, (x + 1) % 4, y), piece_at(zh, (x + 3) % 4, y)
    yp, ym = piece_at(zh, x, (y + 1) % 4), piece_at(zh, x, (y + 3) % 4)
    zo = piece_at(1 - zh, x, y)

    w_copy(me, None, 6, zo, w_own).start()
    w_copy(me, None, 2, yp, w_own).start()
    w_copy(me, None, 3, ym, w_own).start()
    w_copy(me, None, 0, xp, w_own).start()
    w_copy(me, None, 1, xm, w_own).start()
    for arr in range(2):

        @pl.when(z < 3)
        def _():
            to(arr, t, 0, ins[arr]).start()

        @pl.when(z > 0)
        def _():
            to(arr, t, 1, ins[arr]).start()

        to(arr, t, 2, ins[arr]).start()
    own_copies = [
        pltpu.make_async_copy(x_in, rows_of(0, t), local.at[0]),
        pltpu.make_async_copy(g_in, rows_of(1, t), local.at[1]),
        pltpu.make_async_copy(w_own, w_out.at[:, me], local.at[2]),
    ]
    for copy in own_copies:
        copy.start()

    def along_y(h):
        base = h * 16 + x * 4
        near, far, opp = base + (y + 3) % 4, base + (y + 1) % 4, base + (y + 2) % 4
        w_copy(near, None, 0, me).wait_recv()
        w_copy(near, 0, 2, yp).start()
        w_copy(near, None, 0, xp).start()
        w_copy(near, None, 1, xm).start()
        w_copy(far, None, 0, me).wait_recv()
        w_copy(far, 1, 3, ym).start()
        w_copy(far, None, 0, xp).start()
        w_copy(far, None, 1, xm).start()
        w_copy(opp, 0, 0, me).wait_recv()
        w_copy(opp, 1, 0, me).wait_recv()
        w_copy(opp, None, 0, xp).start()
        w_copy(opp, None, 1, xm).start()

    def along_x(h):
        for dy in (0, 3, 1, 2):
            yy = (y + dy) % 4
            near = h * 16 + ((x + 3) % 4) * 4 + yy
            far = h * 16 + ((x + 1) % 4) * 4 + yy
            w_copy(near, None, 0, me).wait_recv()
            w_copy(near, 0, 4, xp).start()
            w_copy(far, None, 0, me).wait_recv()
            w_copy(far, 1, 5, xm).start()

    def along_z(n, arr):
        @pl.when(z - n >= 0)
        def _():
            shard = t - 2 * n
            act_copy(arr, shard, 0, rows_of(arr, shard), t).wait_recv()

            @pl.when(z < 3)
            def _():
                to(arr, shard, 0, rows_of(arr, shard)).start()

            to(arr, shard, 2, rows_of(arr, shard)).start()

        @pl.when(z + n <= 3)
        def _():
            shard = t + 2 * n
            act_copy(arr, shard, 0, rows_of(arr, shard), t).wait_recv()

            @pl.when(z > 0)
            def _():
                to(arr, shard, 1, rows_of(arr, shard)).start()

            to(arr, shard, 2, rows_of(arr, shard)).start()

    along_y(zh)
    zpiece = zo
    w_copy(zpiece, None, 0, me).wait_recv()
    w_copy(zpiece, None, 2, yp).start()
    w_copy(zpiece, None, 3, ym).start()
    w_copy(zpiece, None, 0, xp).start()
    w_copy(zpiece, None, 1, xm).start()
    along_z(1, 0)
    along_y(1 - zh)
    along_z(1, 1)
    along_x(zh)
    along_z(2, 0)
    along_x(1 - zh)
    along_z(2, 1)
    along_z(3, 0)
    along_z(3, 1)

    for zz in range(4):
        for arr in range(2):
            act_copy(arr, zz * 2 + 1 - c, 0, rows_of(arr, zz * 2 + 1 - c), t).wait_recv()
    for h in range(2):
        for yy in range(4):
            opp = h * 16 + ((x + 2) % 4) * 4 + yy
            w_copy(opp, 0, 0, me).wait_recv()
            w_copy(opp, 1, 0, me).wait_recv()
    for copy in own_copies:
        copy.wait()

    for arr in range(2):
        for zz in range(4):
            shard = zz * 2 + c

            @pl.when((zz <= z) & (z < 3))
            def _():
                to(arr, shard, 0, ins[arr]).wait_send()

            @pl.when((zz >= z) & (z > 0))
            def _():
                to(arr, shard, 1, ins[arr]).wait_send()

            to(arr, shard, 2, ins[arr]).wait_send()
    w_copy(me, None, 6, zo, w_own).wait_send()
    for h in range(2):
        base = h * 16 + x * 4
        for dy in range(4):
            yy = (y + dy) % 4
            w_copy(base + yy, None, 0, xp).wait_send()
            w_copy(base + yy, None, 1, xm).wait_send()
            w_copy(h * 16 + ((x + 3) % 4) * 4 + yy, 0, 4, xp).wait_send()
            w_copy(h * 16 + ((x + 1) % 4) * 4 + yy, 1, 5, xm).wait_send()
        w_copy(base + y, None, 2, yp).wait_send()
        w_copy(base + y, None, 3, ym).wait_send()
        w_copy(base + (y + 3) % 4, 0, 2, yp).wait_send()
        w_copy(base + (y + 1) % 4, 1, 3, ym).wait_send()


def gather(counts, tokens, out_grad, tiles):
    return pl.pallas_call(
        gather_kernel,
        name="gather",
        out_shape=(
            jax.ShapeDtypeStruct((8 * ROWS, WIDTH), BF),
            jax.ShapeDtypeStruct((8 * ROWS, WIDTH), BF),
            jax.ShapeDtypeStruct((SLOTS, 32, 4, TILE), BF),
        ),
        in_specs=[SM, ANY, ANY, VM],
        out_specs=(ANY, ANY, ANY),
        scratch_shapes=[
            pltpu.VMEM((SLOTS, 4, TILE), BF),
            pltpu.SemaphoreType.DMA((2, 8, 3)),
            pltpu.SemaphoreType.DMA((2, 8)),
            pltpu.SemaphoreType.DMA((32, 7)),
            pltpu.SemaphoreType.DMA((32, 2)),
            pltpu.SemaphoreType.DMA((3,)),
        ],
        compiler_params=pltpu.CompilerParams(collective_id=0, has_side_effects=True),
    )(counts, tokens, out_grad, tiles)


def dot(a, b, dims):
    return lax.dot_general(a, b, (dims, ((), ())), preferred_element_type=F32)


def block_kernel(scale, counts, rows, x, g, w, f_out, i_out, tg, acc_f, acc_i):
    acc_f[...] = jnp.zeros_like(acc_f)
    acc_i[...] = jnp.zeros_like(acc_i)

    def column(ref, r):
        return ref.at[:, pl.ds(pl.multiple_of(r * TILE, TILE), TILE)]

    def step(j, offsets):
        tiles, blocks, live, where = [], [], [], []
        for m in range(3):
            n = counts[m, j]
            src = x if m < 2 else g
            tiles.append([])
            blocks.append([])
            live.append([])
            where.append([])
            for k in range(3):
                on = k < n
                r = rows[m * 3 + k, j]
                at = m * CAP + offsets[m] + k
                tile = w[jnp.minimum(at, SLOTS - 1)]
                if k:
                    tile = jnp.where(on, tile, jnp.zeros_like(tile))
                tiles[m].append(tile)
                blocks[m].append(column(src, r)[...])
                live[m].append(on)
                where[m].append((r, at))
        x0 = jnp.concatenate(blocks[0], axis=1)
        x1 = jnp.concatenate(blocks[1], axis=1)
        g2 = jnp.concatenate(blocks[2], axis=1)
        w0 = jnp.concatenate(tiles[0], axis=0)
        w1 = jnp.concatenate(tiles[1], axis=0)
        w2 = jnp.concatenate(tiles[2], axis=1)
        gate = dot(x0, w0, ((1,), (0,)))
        up = dot(x1, w1, ((1,), (0,)))
        dh = dot(g2, w2, ((1,), (1,)))
        sig = jax.nn.sigmoid(gate)
        act = gate * sig
        hidden = (act * up).astype(BF)
        d_gate = (dh * up * sig * (1.0 + gate * (1.0 - sig))).astype(BF)
        d_up = (dh * act).astype(BF)
        for m, (value, acc) in enumerate(((d_gate, acc_i), (d_up, acc_i), (hidden, acc_f))):
            wide = dot(value, (w0, w1, w2)[m], ((1,), (1 if m < 2 else 0,)))
            if m < 2:
                terms = dot((x0, x1)[m], value, ((0,), (0,))) * scale
            else:
                terms = dot(value, g2, ((0,), (0,))) * scale
            for k in range(3):
                r, at = where[m][k]

                def put():
                    column(acc, r)[...] += wide[:, k * TILE : (k + 1) * TILE]
                    part = (
                        terms[k * TILE : (k + 1) * TILE]
                        if m < 2
                        else terms[:, k * TILE : (k + 1) * TILE]
                    )
                    tg[at] = part.astype(BF)

                if k:
                    pl.when(live[m][k])(put)
                else:
                    put()
        return tuple(offsets[m] + counts[m, j] for m in range(3))

    lax.fori_loop(0, BLOCKS, step, (jnp.int32(0),) * 3)
    f_out[...] = acc_f[...].astype(BF)
    i_out[...] = acc_i[...].astype(BF)


def compute(counts, rows, x, g, w, scale):
    return pl.pallas_call(
        functools.partial(block_kernel, scale),
        name="blocks",
        out_shape=(
            jax.ShapeDtypeStruct(x.shape, BF),
            jax.ShapeDtypeStruct(x.shape, BF),
            jax.ShapeDtypeStruct((SLOTS, TILE, TILE), BF),
        ),
        in_specs=[SM, SM, VM, VM, VM],
        out_specs=(VM, VM, VM),
        scratch_shapes=[pltpu.VMEM(x.shape, F32), pltpu.VMEM(x.shape, F32)],
        compiler_params=pltpu.CompilerParams(vmem_limit_bytes=56 * 1024 * 1024),
    )(counts, rows, x, g, w)


def scatter_kernel(
    counts,
    f_in,
    i_in,
    tg,
    f_out,
    i_out,
    w_out,
    own,
    mate_in,
    from_left,
    from_right,
    total,
    tx0,
    tx1,
    tx2,
    xa,
    xb,
    xs_lo,
    xs_hi,
    xl,
    xr,
    yb,
    ya,
    yc,
    ys_lo,
    ys_hi,
    yl,
    yr,
    z_own,
    z_send,
    z_in,
    z_sum,
    act_local,
    act_mate_s,
    act_mate_r,
    act_send,
    act_left,
    act_right,
    x_local,
    x_send,
    x_recv,
    y_send,
    y_recv,
    z_sems,
):
    zh, x, y, z, c = places()
    t = z * 2 + c
    ins, outs = (f_in, i_in), (f_out, i_out)
    greet(zh, x, y, z, c)
    lo, hi = pl.ds(0, HALF), pl.ds(HALF, HALF)
    xp, xm = piece_at(zh, (x + 1) % 4, y), piece_at(zh, (x + 3) % 4, y)
    yp, ym = piece_at(zh, x, (y + 1) % 4), piece_at(zh, x, (y + 3) % 4)
    zo = piece_at(1 - zh, x, y)

    def remote(src, dst, send, recv, peer):
        return pltpu.make_async_remote_copy(
            src_ref=src,
            dst_ref=dst,
            send_sem=send,
            recv_sem=recv,
            device_id=peer,
            device_id_type=MESH,
        )

    def rows_of(arr, shard):
        return ins[arr].at[pl.ds(pl.multiple_of(shard * ROWS, ROWS), ROWS)]

    def mate_copy(arr, zz):
        return remote(
            rows_of(arr, zz * 2 + 1 - c),
            mate_in.at[arr, zz],
            act_mate_s.at[arr, zz],
            act_mate_r.at[arr, zz],
            {"tensor": z * 2 + 1 - c},
        )

    def own_copy(arr, zz):
        return pltpu.make_async_copy(
            rows_of(arr, zz * 2 + c), own.at[arr, zz], act_local.at[arr, zz]
        )

    def tx_copy(n):
        return pltpu.make_async_copy(tg.at[:, :, (x + (3, 1, 0)[n]) % 4], (tx0, tx1, tx2)[n], x_local.at[n])

    px, mx = {"dp": xp}, {"dp": xm}
    opp, fwd, bwd = (x + 2) % 4, (x + 1) % 4, (x + 3) % 4
    x_copies = [
        remote(tg.at[lo, :, opp], xa, x_send.at[0], x_recv.at[0], px),
        remote(tg.at[hi, :, opp], xb, x_send.at[1], x_recv.at[1], mx),
        remote(tg.at[hi, :, fwd], xl.at[hi], x_send.at[2], x_recv.at[2], px),
        remote(tg.at[lo, :, bwd], xr.at[lo], x_send.at[3], x_recv.at[3], mx),
        remote(xs_lo, xl.at[lo], x_send.at[4], x_recv.at[4], px),
        remote(xs_hi, xr.at[hi], x_send.at[5], x_recv.at[5], mx),
    ]
    for n in range(4):
        x_copies[n].start()
    order = ((0, 3), (0, 0), (1, 3), (1, 0), (0, 2), (0, 1), (1, 2), (1, 1))
    for arr, zz in order:
        mate_copy(arr, zz).start()
        own_copy(arr, zz).start()
    for n in range(3):
        tx_copy(n).start()

    def along(arr, zz, buf, sems, way, has):
        own_copy(arr, zz).wait()
        mate_copy(arr, zz).wait_recv()

        @pl.when(has)
        def _():
            remote(
                total.at[arr, zz], buf.at[arr, zz], act_send.at[arr, zz], sems.at[arr, zz],
                {"tensor": t},
            ).wait_recv()
            chunks(total, (own, mate_in, buf), arr, zz)

        @pl.when(jnp.logical_not(has))
        def _():
            chunks(total, (own, mate_in), arr, zz)

        remote(
            total.at[arr, zz], buf.at[arr, zz], act_send.at[arr, zz], sems.at[arr, zz],
            {"tensor": t + way},
        ).start()

    def chunks(dst, srcs, *lead):
        for n in range(0, WIDTH, 512):
            s = pl.ds(n, 512)
            at = (*lead, slice(None), s)
            acc = srcs[0][at].astype(F32)
            for src in srcs[1:]:
                acc = acc + src[at].astype(F32)
            if dst is total:
                dst[at] = acc.astype(BF)
            else:
                dst[:, s] = acc.astype(BF)

    def flows(arr, n):
        zz = 3 - n

        @pl.when(z < zz)
        def _():
            along(arr, zz, from_left, act_left, 2, z > 0)

        @pl.when(z > n)
        def _():
            along(arr, n, from_right, act_right, -2, z < 3)

    def each(n, body):
        def step(i, _):
            body(i)
            return 0

        lax.fori_loop(0, n, step, 0)

    flows(0, 0)
    flows(1, 0)

    tx_copy(1).wait()
    x_copies[0].wait_recv()

    def add_lo(i):
        for h in range(2):
            xs_lo[i, h] = (tx1[i, h].astype(F32) + xa[i, h].astype(F32)).astype(BF)

    each(HALF, add_lo)
    x_copies[4].start()
    tx_copy(0).wait()
    x_copies[1].wait_recv()

    def add_hi(i):
        for h in range(2):
            xs_hi[i, h] = (tx0[HALF + i, h].astype(F32) + xb[i, h].astype(F32)).astype(BF)

    each(HALF, add_hi)
    x_copies[5].start()
    flows(0, 1)
    flows(1, 1)

    tx_copy(2).wait()
    for n in (2, 3, 4, 5):
        x_copies[n].wait_recv()

    def x_final(i):
        for h in range(2):
            v = tx2[i, h].astype(F32) + xl[i, h].astype(F32) + xr[i, h].astype(F32)
            for q in range(4):
                yb[q, i, h] = v[4 * q : 4 * q + 4].astype(BF)

    each(SLOTS, x_final)
    py, my = {"dp": yp}, {"dp": ym}
    yo, yf, yw = (y + 2) % 4, (y + 1) % 4, (y + 3) % 4
    y_copies = [
        remote(yb.at[yo, lo], ya, y_send.at[0], y_recv.at[0], py),
        remote(yb.at[yo, hi], yc, y_send.at[1], y_recv.at[1], my),
        remote(yb.at[yf, hi], yl.at[hi], y_send.at[2], y_recv.at[2], py),
        remote(yb.at[yw, lo], yr.at[lo], y_send.at[3], y_recv.at[3], my),
        remote(ys_lo, yl.at[lo], y_send.at[4], y_recv.at[4], py),
        remote(ys_hi, yr.at[hi], y_send.at[5], y_recv.at[5], my),
    ]
    for n in range(4):
        y_copies[n].start()
    y_copies[0].wait_recv()

    def add_ylo(i):
        ys_lo[i] = (yb[yf, i].astype(F32) + ya[i].astype(F32)).astype(BF)

    each(HALF, add_ylo)
    y_copies[4].start()
    y_copies[1].wait_recv()

    def add_yhi(i):
        ys_hi[i] = (yb[yw, HALF + i].astype(F32) + yc[i].astype(F32)).astype(BF)

    each(HALF, add_yhi)
    y_copies[5].start()
    for n in (2, 3, 4, 5):
        y_copies[n].wait_recv()

    def y_final(i):
        def of(h):
            return yb[y, i, h].astype(F32) + yl[i, h].astype(F32) + yr[i, h].astype(F32)

        z_own[i] = of(zh)
        z_send[i] = of(1 - zh).astype(BF)

    each(SLOTS, y_final)
    z_copy = remote(z_send, z_in, z_sems.at[0], z_sems.at[1], {"dp": zo})
    z_copy.start()
    flows(0, 2)
    flows(1, 2)
    z_copy.wait_recv()

    def z_final(i):
        z_sum[i] = (z_own[i] + z_in[i].astype(F32)).astype(BF)

    each(SLOTS, z_final)
    for m in range(3):

        def expand(j, base):
            n = counts[m, j]
            for k in range(3):
                v = z_sum[jnp.minimum(base + k, SLOTS - 1)]
                w_out[m * 42 + j * 3 + k] = jnp.where(k < n, v, jnp.zeros_like(v))
            return base + n

        lax.fori_loop(0, BLOCKS, expand, jnp.int32(m * CAP))

    for arr in range(2):
        own_copy(arr, z).wait()
        mate_copy(arr, z).wait_recv()

        @pl.when(z > 0)
        def _():
            remote(
                total.at[arr, z], from_left.at[arr, z], act_send.at[arr, z], act_left.at[arr, z],
                {"tensor": t},
            ).wait_recv()

        @pl.when(z < 3)
        def _():
            remote(
                total.at[arr, z], from_right.at[arr, z], act_send.at[arr, z], act_right.at[arr, z],
                {"tensor": t},
            ).wait_recv()

    for arr in range(2):
        base = (own, mate_in)
        for has_left, has_right in ((False, True), (True, True), (True, False)):
            here = (z == 0) if not has_left else ((z == 3) if not has_right else (z > 0) & (z < 3))
            bufs = base + ((from_left,) if has_left else ()) + ((from_right,) if has_right else ())

            @pl.when(here)
            def _():
                chunks(outs[arr], bufs, arr, z)

    for arr in range(2):
        for zz in range(4):
            mate_copy(arr, zz).wait_send()

            @pl.when(z != zz)
            def _():
                remote(
                    total.at[arr, zz],
                    from_left.at[arr, zz],
                    act_send.at[arr, zz],
                    act_left.at[arr, zz],
                    {"tensor": t},
                ).wait_send()

    for copy in x_copies + y_copies + [z_copy]:
        copy.wait_send()


def scatter(counts, f, i, tg):
    act = pltpu.VMEM((2, 4, ROWS, WIDTH), BF)
    dma = pltpu.SemaphoreType.DMA
    return pl.pallas_call(
        scatter_kernel,
        name="scatter",
        out_shape=(
            jax.ShapeDtypeStruct((ROWS, WIDTH), BF),
            jax.ShapeDtypeStruct((ROWS, WIDTH), BF),
            jax.ShapeDtypeStruct((3 * 42, 4, TILE), BF),
        ),
        in_specs=[SM, ANY, ANY, ANY],
        out_specs=(VM, VM, VM),
        scratch_shapes=[act] * 5
        + [pltpu.VMEM((SLOTS, 2, 16, TILE), BF)] * 3
        + [pltpu.VMEM((HALF, 2, 16, TILE), BF)] * 4
        + [pltpu.VMEM((SLOTS, 2, 16, TILE), BF)] * 2
        + [pltpu.VMEM((4, SLOTS, 2, 4, TILE), BF)]
        + [pltpu.VMEM((HALF, 2, 4, TILE), BF)] * 4
        + [pltpu.VMEM((SLOTS, 2, 4, TILE), BF)] * 2
        + [pltpu.VMEM((SLOTS, 4, TILE), F32)]
        + [pltpu.VMEM((SLOTS, 4, TILE), BF)] * 3
        + [dma((2, 4))] * 6
        + [dma((3,)), dma((6,)), dma((6,)), dma((6,)), dma((6,)), dma((2,))],
        compiler_params=pltpu.CompilerParams(
            collective_id=1, has_side_effects=True, vmem_limit_bytes=56 * 1024 * 1024
        ),
    )(counts, f, i, tg)


def shards(tokens, out_grad, weight_tiles, tile_counts, tile_rows):
    scale = 1.0 / math.sqrt(8192)
    tiles = weight_tiles.transpose(1, 2, 3, 0, 4).reshape(126, 4, TILE)
    rows = tile_rows.transpose(0, 2, 1).reshape(9, BLOCKS)
    x, g, w = gather(tile_counts, tokens, out_grad, tiles)
    f, i, tg = compute(tile_counts, rows, x, g, w.reshape(SLOTS, TILE, TILE), scale)
    f, i, tg = scatter(tile_counts, f, i, tg.reshape(SLOTS, 2, 4, 16, TILE))
    tile_grad = tg.reshape(3, BLOCKS, 3, 4, TILE).transpose(3, 0, 1, 2, 4)
    return (f, i, tile_grad)


def solution(mesh):
    return jax.shard_map(
        shards,
        mesh=mesh,
        in_specs=(
            P(("dp", "tensor"), None),
            P(("dp", "tensor"), None),
            P("dp", None, "tensor", None, None),
            P(None, "tensor"),
            P(None, "tensor", None),
        ),
        out_specs=(
            P(("dp", "tensor"), None),
            P(("dp", "tensor"), None),
            P("dp", None, "tensor", None, None),
        ),
        check_vma=False,
    )
```

```python
import functools
import math

import jax
import jax.numpy as jnp
from jax import lax
from jax.experimental import pallas as pl
from jax.experimental.pallas import tpu as pltpu
from jax.sharding import PartitionSpec as P

MESH = pl.DeviceIdType.MESH
BF = jnp.bfloat16
F32 = jnp.float32
ANY = pl.BlockSpec(memory_space=pl.ANY)
VM = pl.BlockSpec(memory_space=pltpu.VMEM)
SM = pl.BlockSpec(memory_space=pltpu.SMEM)

CAP = 28
SLOTS = 3 * CAP
HALF = SLOTS // 2
BLOCKS = 14
ROWS = 32
WIDTH = 4096
TILE = 128


def places():
    d = lax.axis_index("dp")
    t = lax.axis_index("tensor")
    return d // 16, (d // 4) % 4, d % 4, t // 2, t % 2


def piece_at(zh, x, y):
    return zh * 16 + x * 4 + y


def greet(zh, x, y, z, c):
    barrier = pltpu.get_barrier_semaphore()
    peers = [
        {"tensor": ((z + 1) % 4) * 2 + c},
        {"tensor": ((z + 3) % 4) * 2 + c},
        {"tensor": z * 2 + 1 - c},
        {"dp": piece_at(zh, x, (y + 1) % 4)},
        {"dp": piece_at(zh, x, (y + 3) % 4)},
        {"dp": piece_at(zh, (x + 1) % 4, y)},
        {"dp": piece_at(zh, (x + 3) % 4, y)},
        {"dp": piece_at(1 - zh, x, y)},
    ]
    for peer in peers:
        pl.semaphore_signal(barrier, inc=1, device_id=peer, device_id_type=MESH)
    pl.semaphore_wait(barrier, len(peers))


def gather_kernel(
    counts, x_in, g_in, w_in, x_out, g_out, w_out, w_own, xs_send, xs_recv, w_send, w_recv, local
):
    zh, x, y, z, c = places()
    t = z * 2 + c
    ins, outs = (x_in, g_in), (x_out, g_out)
    greet(zh, x, y, z, c)

    def rows_of(arr, shard):
        return outs[arr].at[pl.ds(pl.multiple_of(shard * ROWS, ROWS), ROWS)]

    def act_copy(arr, shard, way, src, peer):
        return pltpu.make_async_remote_copy(
            src_ref=src,
            dst_ref=rows_of(arr, shard),
            send_sem=xs_send.at[arr, shard, way],
            recv_sem=xs_recv.at[arr, shard],
            device_id={"tensor": peer},
            device_id_type=MESH,
        )

    right, left, mate = t + 2, t - 2, z * 2 + 1 - c

    def to(arr, shard, way, src):
        return act_copy(arr, shard, way, src, (right, left, mate)[way])

    def compact(m):
        def step(i, carry):
            j, k = carry
            w_own[m * CAP + i] = w_in[m * 42 + j * 3 + k]
            more = k + 1 < counts[m, j]
            return (
                jnp.where(more, j, jnp.minimum(j + 1, BLOCKS - 1)),
                jnp.where(more, k + 1, 0),
            )

        lax.fori_loop(0, CAP, step, (jnp.int32(0), jnp.int32(0)))

    for m in range(3):
        compact(m)

    me = piece_at(zh, x, y)
    halves = (pl.ds(0, HALF), pl.ds(HALF, HALF))

    def w_part(piece, half):
        if half is None:
            return w_out.at[:, piece]
        return w_out.at[halves[half], piece]

    def w_copy(piece, half, way, peer, src=None):
        return pltpu.make_async_remote_copy(
            src_ref=w_part(piece, half) if src is None else src,
            dst_ref=w_part(piece, half),
            send_sem=w_send.at[piece, way],
            recv_sem=w_recv.at[piece, 1 if half == 1 else 0],
            device_id={"dp": peer},
            device_id_type=MESH,
        )

    xp, xm = piece_at(zh, (x + 1) % 4, y), piece_at(zh, (x + 3) % 4, y)
    yp, ym = piece_at(zh, x, (y + 1) % 4), piece_at(zh, x, (y + 3) % 4)
    zo = piece_at(1 - zh, x, y)

    w_copy(me, None, 6, zo, w_own).start()
    w_copy(me, None, 2, yp, w_own).start()
    w_copy(me, None, 3, ym, w_own).start()
    w_copy(me, None, 0, xp, w_own).start()
    w_copy(me, None, 1, xm, w_own).start()
    for arr in range(2):

        @pl.when(z < 3)
        def _():
            to(arr, t, 0, ins[arr]).start()

        @pl.when(z > 0)
        def _():
            to(arr, t, 1, ins[arr]).start()

        to(arr, t, 2, ins[arr]).start()
    own_copies = [
        pltpu.make_async_copy(x_in, rows_of(0, t), local.at[0]),
        pltpu.make_async_copy(g_in, rows_of(1, t), local.at[1]),
        pltpu.make_async_copy(w_own, w_out.at[:, me], local.at[2]),
    ]
    for copy in own_copies:
        copy.start()

    def along_y(h):
        base = h * 16 + x * 4
        near, far, opp = base + (y + 3) % 4, base + (y + 1) % 4, base + (y + 2) % 4
        w_copy(near, None, 0, me).wait_recv()
        w_copy(near, 0, 2, yp).start()
        w_copy(near, None, 0, xp).start()
        w_copy(near, None, 1, xm).start()
        w_copy(far, None, 0, me).wait_recv()
        w_copy(far, 1, 3, ym).start()
        w_copy(far, None, 0, xp).start()
        w_copy(far, None, 1, xm).start()
        w_copy(opp, 0, 0, me).wait_recv()
        w_copy(opp, 1, 0, me).wait_recv()
        w_copy(opp, None, 0, xp).start()
        w_copy(opp, None, 1, xm).start()

    def along_x(h):
        for dy in (0, 3, 1, 2):
            yy = (y + dy) % 4
            near = h * 16 + ((x + 3) % 4) * 4 + yy
            far = h * 16 + ((x + 1) % 4) * 4 + yy
            w_copy(near, None, 0, me).wait_recv()
            w_copy(near, 0, 4, xp).start()
            w_copy(far, None, 0, me).wait_recv()
            w_copy(far, 1, 5, xm).start()

    def along_z(n, arr):
        @pl.when(z - n >= 0)
        def _():
            shard = t - 2 * n
            act_copy(arr, shard, 0, rows_of(arr, shard), t).wait_recv()

            @pl.when(z < 3)
            def _():
                to(arr, shard, 0, rows_of(arr, shard)).start()

            to(arr, shard, 2, rows_of(arr, shard)).start()

        @pl.when(z + n <= 3)
        def _():
            shard = t + 2 * n
            act_copy(arr, shard, 0, rows_of(arr, shard), t).wait_recv()

            @pl.when(z > 0)
            def _():
                to(arr, shard, 1, rows_of(arr, shard)).start()

            to(arr, shard, 2, rows_of(arr, shard)).start()

    along_y(zh)
    zpiece = zo
    w_copy(zpiece, None, 0, me).wait_recv()
    w_copy(zpiece, None, 2, yp).start()
    w_copy(zpiece, None, 3, ym).start()
    w_copy(zpiece, None, 0, xp).start()
    w_copy(zpiece, None, 1, xm).start()
    along_z(1, 0)
    along_y(1 - zh)
    along_z(1, 1)
    along_x(zh)
    along_z(2, 0)
    along_x(1 - zh)
    along_z(2, 1)
    along_z(3, 0)
    along_z(3, 1)

    for zz in range(4):
        for arr in range(2):
            act_copy(arr, zz * 2 + 1 - c, 0, rows_of(arr, zz * 2 + 1 - c), t).wait_recv()
    for h in range(2):
        for yy in range(4):
            opp = h * 16 + ((x + 2) % 4) * 4 + yy
            w_copy(opp, 0, 0, me).wait_recv()
            w_copy(opp, 1, 0, me).wait_recv()
    for copy in own_copies:
        copy.wait()

    for arr in range(2):
        for zz in range(4):
            shard = zz * 2 + c

            @pl.when((zz <= z) & (z < 3))
            def _():
                to(arr, shard, 0, ins[arr]).wait_send()

            @pl.when((zz >= z) & (z > 0))
            def _():
                to(arr, shard, 1, ins[arr]).wait_send()

            to(arr, shard, 2, ins[arr]).wait_send()
    w_copy(me, None, 6, zo, w_own).wait_send()
    for h in range(2):
        base = h * 16 + x * 4
        for dy in range(4):
            yy = (y + dy) % 4
            w_copy(base + yy, None, 0, xp).wait_send()
            w_copy(base + yy, None, 1, xm).wait_send()
            w_copy(h * 16 + ((x + 3) % 4) * 4 + yy, 0, 4, xp).wait_send()
            w_copy(h * 16 + ((x + 1) % 4) * 4 + yy, 1, 5, xm).wait_send()
        w_copy(base + y, None, 2, yp).wait_send()
        w_copy(base + y, None, 3, ym).wait_send()
        w_copy(base + (y + 3) % 4, 0, 2, yp).wait_send()
        w_copy(base + (y + 1) % 4, 1, 3, ym).wait_send()


def gather(counts, tokens, out_grad, tiles):
    return pl.pallas_call(
        gather_kernel,
        name="gather",
        out_shape=(
            jax.ShapeDtypeStruct((8 * ROWS, WIDTH), BF),
            jax.ShapeDtypeStruct((8 * ROWS, WIDTH), BF),
            jax.ShapeDtypeStruct((SLOTS, 32, 4, TILE), BF),
        ),
        in_specs=[SM, ANY, ANY, VM],
        out_specs=(ANY, ANY, ANY),
        scratch_shapes=[
            pltpu.VMEM((SLOTS, 4, TILE), BF),
            pltpu.SemaphoreType.DMA((2, 8, 3)),
            pltpu.SemaphoreType.DMA((2, 8)),
            pltpu.SemaphoreType.DMA((32, 7)),
            pltpu.SemaphoreType.DMA((32, 2)),
            pltpu.SemaphoreType.DMA((3,)),
        ],
        compiler_params=pltpu.CompilerParams(collective_id=0, has_side_effects=True),
    )(counts, tokens, out_grad, tiles)


def dot(a, b, dims):
    return lax.dot_general(a, b, (dims, ((), ())), preferred_element_type=F32)


def block_kernel(scale, counts, rows, x, g, w, f_out, i_out, tg, acc_f, acc_i):
    acc_f[...] = jnp.zeros_like(acc_f)
    acc_i[...] = jnp.zeros_like(acc_i)

    def column(ref, r):
        return ref.at[:, pl.ds(pl.multiple_of(r * TILE, TILE), TILE)]

    def step(j, offsets):
        tiles, blocks, live, where = [], [], [], []
        for m in range(3):
            n = counts[m, j]
            src = x if m < 2 else g
            tiles.append([])
            blocks.append([])
            live.append([])
            where.append([])
            for k in range(3):
                on = k < n
                r = rows[m, k, j]
                at = m * CAP + offsets[m] + k
                tile = w[jnp.minimum(at, SLOTS - 1)]
                if k:
                    tile = jnp.where(on, tile, jnp.zeros_like(tile))
                tiles[m].append(tile)
                blocks[m].append(column(src, r)[...])
                live[m].append(on)
                where[m].append((r, at))
        x0 = jnp.concatenate(blocks[0], axis=1)
        x1 = jnp.concatenate(blocks[1], axis=1)
        g2 = jnp.concatenate(blocks[2], axis=1)
        w0 = jnp.concatenate(tiles[0], axis=0)
        w1 = jnp.concatenate(tiles[1], axis=0)
        w2 = jnp.concatenate(tiles[2], axis=1)
        gate = dot(x0, w0, ((1,), (0,)))
        up = dot(x1, w1, ((1,), (0,)))
        dh = dot(g2, w2, ((1,), (1,)))
        sig = jax.nn.sigmoid(gate)
        act = gate * sig
        hidden = (act * up).astype(BF)
        d_gate = (dh * up * sig * (1.0 + gate * (1.0 - sig))).astype(BF)
        d_up = (dh * act).astype(BF)
        for m, (value, acc) in enumerate(((d_gate, acc_i), (d_up, acc_i), (hidden, acc_f))):
            wide = dot(value, (w0, w1, w2)[m], ((1,), (1 if m < 2 else 0,)))
            if m < 2:
                terms = dot((x0, x1)[m], value, ((0,), (0,))) * scale
            else:
                terms = dot(value, g2, ((0,), (0,))) * scale
            for k in range(3):
                r, at = where[m][k]

                def put():
                    column(acc, r)[...] += wide[:, k * TILE : (k + 1) * TILE]
                    part = (
                        terms[k * TILE : (k + 1) * TILE]
                        if m < 2
                        else terms[:, k * TILE : (k + 1) * TILE]
                    )
                    tg[at] = part.astype(BF)

                if k:
                    pl.when(live[m][k])(put)
                else:
                    put()
        return tuple(offsets[m] + counts[m, j] for m in range(3))

    lax.fori_loop(0, BLOCKS, step, (jnp.int32(0),) * 3)
    f_out[...] = acc_f[...].astype(BF)
    i_out[...] = acc_i[...].astype(BF)


def compute(counts, rows, x, g, w, scale):
    return pl.pallas_call(
        functools.partial(block_kernel, scale),
        name="blocks",
        out_shape=(
            jax.ShapeDtypeStruct(x.shape, BF),
            jax.ShapeDtypeStruct(x.shape, BF),
            jax.ShapeDtypeStruct((SLOTS, TILE, TILE), BF),
        ),
        in_specs=[SM, SM, VM, VM, VM],
        out_specs=(VM, VM, VM),
        scratch_shapes=[pltpu.VMEM(x.shape, F32), pltpu.VMEM(x.shape, F32)],
        compiler_params=pltpu.CompilerParams(vmem_limit_bytes=56 * 1024 * 1024),
    )(counts, rows, x, g, w)


def scatter_kernel(
    f_in,
    i_in,
    tg,
    f_out,
    i_out,
    w_out,
    own,
    mate_in,
    from_left,
    from_right,
    total,
    tx0,
    tx1,
    tx2,
    xa,
    xb,
    xs_lo,
    xs_hi,
    xl,
    xr,
    yb,
    ya,
    yc,
    ys_lo,
    ys_hi,
    yl,
    yr,
    z_own,
    z_send,
    z_in,
    act_local,
    act_mate_s,
    act_mate_r,
    act_send,
    act_left,
    act_right,
    x_local,
    x_send,
    x_recv,
    y_send,
    y_recv,
    z_sems,
):
    zh, x, y, z, c = places()
    t = z * 2 + c
    ins, outs = (f_in, i_in), (f_out, i_out)
    greet(zh, x, y, z, c)
    lo, hi = pl.ds(0, HALF), pl.ds(HALF, HALF)
    xp, xm = piece_at(zh, (x + 1) % 4, y), piece_at(zh, (x + 3) % 4, y)
    yp, ym = piece_at(zh, x, (y + 1) % 4), piece_at(zh, x, (y + 3) % 4)
    zo = piece_at(1 - zh, x, y)

    def remote(src, dst, send, recv, peer):
        return pltpu.make_async_remote_copy(
            src_ref=src,
            dst_ref=dst,
            send_sem=send,
            recv_sem=recv,
            device_id=peer,
            device_id_type=MESH,
        )

    def rows_of(arr, shard):
        return ins[arr].at[pl.ds(pl.multiple_of(shard * ROWS, ROWS), ROWS)]

    def mate_copy(arr, zz):
        return remote(
            rows_of(arr, zz * 2 + 1 - c),
            mate_in.at[arr, zz],
            act_mate_s.at[arr, zz],
            act_mate_r.at[arr, zz],
            {"tensor": z * 2 + 1 - c},
        )

    def own_copy(arr, zz):
        return pltpu.make_async_copy(
            rows_of(arr, zz * 2 + c), own.at[arr, zz], act_local.at[arr, zz]
        )

    def tx_copy(n):
        return pltpu.make_async_copy(tg.at[:, :, (x + (3, 1, 0)[n]) % 4], (tx0, tx1, tx2)[n], x_local.at[n])

    px, mx = {"dp": xp}, {"dp": xm}
    opp, fwd, bwd = (x + 2) % 4, (x + 1) % 4, (x + 3) % 4
    x_copies = [
        remote(tg.at[lo, :, opp], xa, x_send.at[0], x_recv.at[0], px),
        remote(tg.at[hi, :, opp], xb, x_send.at[1], x_recv.at[1], mx),
        remote(tg.at[hi, :, fwd], xl.at[hi], x_send.at[2], x_recv.at[2], px),
        remote(tg.at[lo, :, bwd], xr.at[lo], x_send.at[3], x_recv.at[3], mx),
        remote(xs_lo, xl.at[lo], x_send.at[4], x_recv.at[4], px),
        remote(xs_hi, xr.at[hi], x_send.at[5], x_recv.at[5], mx),
    ]
    for n in range(4):
        x_copies[n].start()
    order = ((0, 3), (0, 0), (1, 3), (1, 0), (0, 2), (0, 1), (1, 2), (1, 1))
    for arr, zz in order:
        mate_copy(arr, zz).start()
        own_copy(arr, zz).start()
    for n in range(3):
        tx_copy(n).start()

    def along(arr, zz, buf, sems, way, first):
        own_copy(arr, zz).wait()
        mate_copy(arr, zz).wait_recv()
        hop = remote(
            total.at[arr, zz], buf.at[arr, zz], act_send.at[arr, zz], sems.at[arr, zz],
            {"tensor": t + way},
        )
        if first:
            chunks(total, (own, mate_in), arr, zz)
        else:
            hop.wait_recv()
            chunks(total, (own, mate_in, buf), arr, zz)
        hop.start()

    def chunks(dst, srcs, *lead):
        for n in range(0, WIDTH, 512):
            s = pl.ds(n, 512)
            at = (*lead, slice(None), s)
            acc = srcs[0][at].astype(F32)
            for src in srcs[1:]:
                acc = acc + src[at].astype(F32)
            if dst is total:
                dst[at] = acc.astype(BF)
            else:
                dst[:, s] = acc.astype(BF)

    def ends():
        @pl.when(z == 0)
        def _():
            for zz in (3, 2, 1):
                for arr in range(2):
                    along(arr, zz, from_left, act_left, 2, True)

        @pl.when(z == 3)
        def _():
            for zz in (0, 1, 2):
                for arr in range(2):
                    along(arr, zz, from_right, act_right, -2, True)

    def middle(arr, n):
        @pl.when(z == 1)
        def _():
            if n < 2:
                along(arr, 3 - n, from_left, act_left, 2, False)
            else:
                along(arr, 0, from_right, act_right, -2, False)

        @pl.when(z == 2)
        def _():
            if n < 2:
                along(arr, n, from_right, act_right, -2, False)
            else:
                along(arr, 3, from_left, act_left, 2, False)

    def final(arr):
        own_copy(arr, z).wait()
        mate_copy(arr, z).wait_recv()

        @pl.when(z > 0)
        def _():
            remote(
                total.at[arr, z], from_left.at[arr, z], act_send.at[arr, z], act_left.at[arr, z],
                {"tensor": t},
            ).wait_recv()

        @pl.when(z < 3)
        def _():
            remote(
                total.at[arr, z], from_right.at[arr, z], act_send.at[arr, z], act_right.at[arr, z],
                {"tensor": t},
            ).wait_recv()

        base = (own, mate_in)
        for has_left, has_right in ((False, True), (True, True), (True, False)):
            here = (z == 0) if not has_left else ((z == 3) if not has_right else (z > 0) & (z < 3))
            bufs = base + ((from_left,) if has_left else ()) + ((from_right,) if has_right else ())

            @pl.when(here)
            def _():
                chunks(outs[arr], bufs, arr, z)

    def each(n, body):
        def step(i, _):
            body(i)
            return 0

        lax.fori_loop(0, n, step, 0)

    ends()
    middle(0, 0)

    tx_copy(1).wait()
    x_copies[0].wait_recv()

    def add_lo(i):
        for h in range(2):
            xs_lo[i, h] = (tx1[i, h].astype(F32) + xa[i, h].astype(F32)).astype(BF)

    each(HALF, add_lo)
    x_copies[4].start()
    tx_copy(0).wait()
    x_copies[1].wait_recv()

    def add_hi(i):
        for h in range(2):
            xs_hi[i, h] = (tx0[HALF + i, h].astype(F32) + xb[i, h].astype(F32)).astype(BF)

    each(HALF, add_hi)
    x_copies[5].start()
    middle(1, 0)
    middle(0, 2)
    middle(0, 1)
    middle(1, 2)

    tx_copy(2).wait()
    for n in (2, 3, 4, 5):
        x_copies[n].wait_recv()

    def x_final(i):
        for h in range(2):
            v = tx2[i, h].astype(F32) + xl[i, h].astype(F32) + xr[i, h].astype(F32)
            for q in range(4):
                yb[q, i, h] = v[4 * q : 4 * q + 4].astype(BF)

    each(SLOTS, x_final)
    py, my = {"dp": yp}, {"dp": ym}
    yo, yf, yw = (y + 2) % 4, (y + 1) % 4, (y + 3) % 4
    y_copies = [
        remote(yb.at[yo, lo], ya, y_send.at[0], y_recv.at[0], py),
        remote(yb.at[yo, hi], yc, y_send.at[1], y_recv.at[1], my),
        remote(yb.at[yf, hi], yl.at[hi], y_send.at[2], y_recv.at[2], py),
        remote(yb.at[yw, lo], yr.at[lo], y_send.at[3], y_recv.at[3], my),
        remote(ys_lo, yl.at[lo], y_send.at[4], y_recv.at[4], py),
        remote(ys_hi, yr.at[hi], y_send.at[5], y_recv.at[5], my),
    ]
    for n in range(4):
        y_copies[n].start()
    middle(1, 1)
    y_copies[0].wait_recv()

    def add_ylo(i):
        ys_lo[i] = (yb[yf, i].astype(F32) + ya[i].astype(F32)).astype(BF)

    each(HALF, add_ylo)
    y_copies[4].start()
    y_copies[1].wait_recv()

    def add_yhi(i):
        ys_hi[i] = (yb[yw, HALF + i].astype(F32) + yc[i].astype(F32)).astype(BF)

    each(HALF, add_yhi)
    y_copies[5].start()
    for n in (2, 3, 4, 5):
        y_copies[n].wait_recv()

    def y_final(i):
        def of(h):
            return yb[y, i, h].astype(F32) + yl[i, h].astype(F32) + yr[i, h].astype(F32)

        z_own[i] = of(zh)
        z_send[i] = of(1 - zh).astype(BF)

    each(SLOTS, y_final)
    z_copy = remote(z_send, z_in, z_sems.at[0], z_sems.at[1], {"dp": zo})
    z_copy.start()
    final(0)
    final(1)
    z_copy.wait_recv()

    def z_final(i):
        w_out[i] = (z_own[i] + z_in[i].astype(F32)).astype(BF)

    each(SLOTS, z_final)
    for arr in range(2):
        for zz in range(4):
            mate_copy(arr, zz).wait_send()

            @pl.when(z != zz)
            def _():
                remote(
                    total.at[arr, zz],
                    from_left.at[arr, zz],
                    act_send.at[arr, zz],
                    act_left.at[arr, zz],
                    {"tensor": t},
                ).wait_send()

    for copy in x_copies + y_copies + [z_copy]:
        copy.wait_send()


def scatter(f, i, tg):
    act = pltpu.VMEM((2, 4, ROWS, WIDTH), BF)
    dma = pltpu.SemaphoreType.DMA
    return pl.pallas_call(
        scatter_kernel,
        name="scatter",
        out_shape=(
            jax.ShapeDtypeStruct((ROWS, WIDTH), BF),
            jax.ShapeDtypeStruct((ROWS, WIDTH), BF),
            jax.ShapeDtypeStruct((SLOTS, 4, TILE), BF),
        ),
        in_specs=[ANY, ANY, ANY],
        out_specs=(VM, VM, VM),
        scratch_shapes=[act] * 5
        + [pltpu.VMEM((SLOTS, 2, 16, TILE), BF)] * 3
        + [pltpu.VMEM((HALF, 2, 16, TILE), BF)] * 4
        + [pltpu.VMEM((SLOTS, 2, 16, TILE), BF)] * 2
        + [pltpu.VMEM((4, SLOTS, 2, 4, TILE), BF)]
        + [pltpu.VMEM((HALF, 2, 4, TILE), BF)] * 4
        + [pltpu.VMEM((SLOTS, 2, 4, TILE), BF)] * 2
        + [pltpu.VMEM((SLOTS, 4, TILE), F32)]
        + [pltpu.VMEM((SLOTS, 4, TILE), BF)] * 2
        + [dma((2, 4))] * 6
        + [dma((3,)), dma((6,)), dma((6,)), dma((6,)), dma((6,)), dma((2,))],
        compiler_params=pltpu.CompilerParams(
            collective_id=1, has_side_effects=True, vmem_limit_bytes=56 * 1024 * 1024
        ),
    )(f, i, tg)


def finish_kernel(counts, f_in, i_in, w_in, f_out, i_out, w_out):
    f_out[...] = f_in[...]
    i_out[...] = i_in[...]
    for m in range(3):

        def expand(j, base):
            n = counts[m, j]
            for k in range(3):
                v = w_in[jnp.minimum(base + k, SLOTS - 1)]
                w_out[m * 42 + j * 3 + k] = jnp.where(k < n, v, jnp.zeros_like(v))
            return base + n

        lax.fori_loop(0, BLOCKS, expand, jnp.int32(m * CAP))


def finish(counts, f, i, tg):
    return pl.pallas_call(
        finish_kernel,
        name="finish",
        out_shape=(
            jax.ShapeDtypeStruct(f.shape, BF),
            jax.ShapeDtypeStruct(i.shape, BF),
            jax.ShapeDtypeStruct((3 * 42, 4, TILE), BF),
        ),
        in_specs=[SM, VM, VM, VM],
        out_specs=(VM, VM, VM),
    )(counts, f, i, tg)


def shards(tokens, out_grad, weight_tiles, tile_counts, tile_rows):
    scale = 1.0 / math.sqrt(8192)
    tiles = weight_tiles.transpose(1, 2, 3, 0, 4).reshape(126, 4, TILE)
    rows = tile_rows.transpose(0, 2, 1)
    x, g, w = gather(tile_counts, tokens, out_grad, tiles)
    f, i, tg = compute(tile_counts, rows, x, g, w.reshape(SLOTS, TILE, TILE), scale)
    f, i, tg = scatter(f, i, tg.reshape(SLOTS, 2, 4, 16, TILE))
    f, i, tg = finish(tile_counts, f, i, tg)
    tile_grad = tg.reshape(3, BLOCKS, 3, 4, TILE).transpose(3, 0, 1, 2, 4)
    return (f, i, tile_grad)


def solution(mesh):
    return jax.shard_map(
        shards,
        mesh=mesh,
        in_specs=(
            P(("dp", "tensor"), None),
            P(("dp", "tensor"), None),
            P("dp", None, "tensor", None, None),
            P(None, "tensor"),
            P(None, "tensor", None),
        ),
        out_specs=(
            P(("dp", "tensor"), None),
            P(("dp", "tensor"), None),
            P("dp", None, "tensor", None, None),
        ),
        check_vma=False,
    )
```

```python
import functools
import math

import jax
import jax.numpy as jnp
from jax import lax
from jax.experimental import pallas as pl
from jax.experimental.pallas import tpu as pltpu
from jax.sharding import PartitionSpec as P

MESH = pl.DeviceIdType.MESH
BF = jnp.bfloat16
F32 = jnp.float32
ANY = pl.BlockSpec(memory_space=pl.ANY)
VM = pl.BlockSpec(memory_space=pltpu.VMEM)
SM = pl.BlockSpec(memory_space=pltpu.SMEM)

CAP = 28
SLOTS = 3 * CAP
HALF = SLOTS // 2
BLOCKS = 14
ROWS = 32
WIDTH = 4096
TILE = 128


def places():
    d = lax.axis_index("dp")
    t = lax.axis_index("tensor")
    return d // 16, (d // 4) % 4, d % 4, t // 2, t % 2


def piece_at(zh, x, y):
    return zh * 16 + x * 4 + y


def greet(zh, x, y, z, c):
    barrier = pltpu.get_barrier_semaphore()
    peers = [
        {"tensor": ((z + 1) % 4) * 2 + c},
        {"tensor": ((z + 3) % 4) * 2 + c},
        {"tensor": z * 2 + 1 - c},
        {"dp": piece_at(zh, x, (y + 1) % 4)},
        {"dp": piece_at(zh, x, (y + 3) % 4)},
        {"dp": piece_at(zh, (x + 1) % 4, y)},
        {"dp": piece_at(zh, (x + 3) % 4, y)},
        {"dp": piece_at(1 - zh, x, y)},
    ]
    for peer in peers:
        pl.semaphore_signal(barrier, inc=1, device_id=peer, device_id_type=MESH)
    pl.semaphore_wait(barrier, len(peers))


def gather_kernel(
    counts, x_in, g_in, w_in, x_out, g_out, w_out, w_own, xs_send, xs_recv, w_send, w_recv, local
):
    zh, x, y, z, c = places()
    t = z * 2 + c
    ins, outs = (x_in, g_in), (x_out, g_out)
    greet(zh, x, y, z, c)

    def rows_of(arr, shard):
        return outs[arr].at[pl.ds(pl.multiple_of(shard * ROWS, ROWS), ROWS)]

    def act_copy(arr, shard, way, src, peer):
        return pltpu.make_async_remote_copy(
            src_ref=src,
            dst_ref=rows_of(arr, shard),
            send_sem=xs_send.at[arr, shard, way],
            recv_sem=xs_recv.at[arr, shard],
            device_id={"tensor": peer},
            device_id_type=MESH,
        )

    right, left, mate = t + 2, t - 2, z * 2 + 1 - c

    def to(arr, shard, way, src):
        return act_copy(arr, shard, way, src, (right, left, mate)[way])

    def compact(m):
        def step(i, carry):
            j, k = carry
            w_own[m * CAP + i] = w_in[m * 42 + j * 3 + k]
            more = k + 1 < counts[m, j]
            return (
                jnp.where(more, j, jnp.minimum(j + 1, BLOCKS - 1)),
                jnp.where(more, k + 1, 0),
            )

        lax.fori_loop(0, CAP, step, (jnp.int32(0), jnp.int32(0)))

    for m in range(3):
        compact(m)

    me = piece_at(zh, x, y)
    halves = (pl.ds(0, HALF), pl.ds(HALF, HALF))

    def w_part(piece, half):
        if half is None:
            return w_out.at[:, piece]
        return w_out.at[halves[half], piece]

    def w_copy(piece, half, way, peer, src=None):
        return pltpu.make_async_remote_copy(
            src_ref=w_part(piece, half) if src is None else src,
            dst_ref=w_part(piece, half),
            send_sem=w_send.at[piece, way],
            recv_sem=w_recv.at[piece, 1 if half == 1 else 0],
            device_id={"dp": peer},
            device_id_type=MESH,
        )

    xp, xm = piece_at(zh, (x + 1) % 4, y), piece_at(zh, (x + 3) % 4, y)
    yp, ym = piece_at(zh, x, (y + 1) % 4), piece_at(zh, x, (y + 3) % 4)
    zo = piece_at(1 - zh, x, y)

    w_copy(me, None, 6, zo, w_own).start()
    w_copy(me, None, 2, yp, w_own).start()
    w_copy(me, None, 3, ym, w_own).start()
    w_copy(me, None, 0, xp, w_own).start()
    w_copy(me, None, 1, xm, w_own).start()
    for arr in range(2):

        @pl.when(z < 3)
        def _():
            to(arr, t, 0, ins[arr]).start()

        @pl.when(z > 0)
        def _():
            to(arr, t, 1, ins[arr]).start()

        to(arr, t, 2, ins[arr]).start()
    own_copies = [
        pltpu.make_async_copy(x_in, rows_of(0, t), local.at[0]),
        pltpu.make_async_copy(g_in, rows_of(1, t), local.at[1]),
        pltpu.make_async_copy(w_own, w_out.at[:, me], local.at[2]),
    ]
    for copy in own_copies:
        copy.start()

    def along_y(h):
        base = h * 16 + x * 4
        near, far, opp = base + (y + 3) % 4, base + (y + 1) % 4, base + (y + 2) % 4
        w_copy(near, None, 0, me).wait_recv()
        w_copy(near, 0, 2, yp).start()
        w_copy(near, None, 0, xp).start()
        w_copy(near, None, 1, xm).start()
        w_copy(far, None, 0, me).wait_recv()
        w_copy(far, 1, 3, ym).start()
        w_copy(far, None, 0, xp).start()
        w_copy(far, None, 1, xm).start()
        w_copy(opp, 0, 0, me).wait_recv()
        w_copy(opp, 1, 0, me).wait_recv()
        w_copy(opp, None, 0, xp).start()
        w_copy(opp, None, 1, xm).start()

    def along_x(h):
        for dy in (0, 3, 1, 2):
            yy = (y + dy) % 4
            near = h * 16 + ((x + 3) % 4) * 4 + yy
            far = h * 16 + ((x + 1) % 4) * 4 + yy
            w_copy(near, None, 0, me).wait_recv()
            w_copy(near, 0, 4, xp).start()
            w_copy(far, None, 0, me).wait_recv()
            w_copy(far, 1, 5, xm).start()

    def along_z(n, arr):
        @pl.when(z - n >= 0)
        def _():
            shard = t - 2 * n
            act_copy(arr, shard, 0, rows_of(arr, shard), t).wait_recv()

            @pl.when(z < 3)
            def _():
                to(arr, shard, 0, rows_of(arr, shard)).start()

            to(arr, shard, 2, rows_of(arr, shard)).start()

        @pl.when(z + n <= 3)
        def _():
            shard = t + 2 * n
            act_copy(arr, shard, 0, rows_of(arr, shard), t).wait_recv()

            @pl.when(z > 0)
            def _():
                to(arr, shard, 1, rows_of(arr, shard)).start()

            to(arr, shard, 2, rows_of(arr, shard)).start()

    along_y(zh)
    zpiece = zo
    w_copy(zpiece, None, 0, me).wait_recv()
    w_copy(zpiece, None, 2, yp).start()
    w_copy(zpiece, None, 3, ym).start()
    w_copy(zpiece, None, 0, xp).start()
    w_copy(zpiece, None, 1, xm).start()
    along_z(1, 0)
    along_y(1 - zh)
    along_z(1, 1)
    along_x(zh)
    along_z(2, 0)
    along_x(1 - zh)
    along_z(2, 1)
    along_z(3, 0)
    along_z(3, 1)

    for zz in range(4):
        for arr in range(2):
            act_copy(arr, zz * 2 + 1 - c, 0, rows_of(arr, zz * 2 + 1 - c), t).wait_recv()
    for h in range(2):
        for yy in range(4):
            opp = h * 16 + ((x + 2) % 4) * 4 + yy
            w_copy(opp, 0, 0, me).wait_recv()
            w_copy(opp, 1, 0, me).wait_recv()
    for copy in own_copies:
        copy.wait()

    for arr in range(2):
        for zz in range(4):
            shard = zz * 2 + c

            @pl.when((zz <= z) & (z < 3))
            def _():
                to(arr, shard, 0, ins[arr]).wait_send()

            @pl.when((zz >= z) & (z > 0))
            def _():
                to(arr, shard, 1, ins[arr]).wait_send()

            to(arr, shard, 2, ins[arr]).wait_send()
    w_copy(me, None, 6, zo, w_own).wait_send()
    for h in range(2):
        base = h * 16 + x * 4
        for dy in range(4):
            yy = (y + dy) % 4
            w_copy(base + yy, None, 0, xp).wait_send()
            w_copy(base + yy, None, 1, xm).wait_send()
            w_copy(h * 16 + ((x + 3) % 4) * 4 + yy, 0, 4, xp).wait_send()
            w_copy(h * 16 + ((x + 1) % 4) * 4 + yy, 1, 5, xm).wait_send()
        w_copy(base + y, None, 2, yp).wait_send()
        w_copy(base + y, None, 3, ym).wait_send()
        w_copy(base + (y + 3) % 4, 0, 2, yp).wait_send()
        w_copy(base + (y + 1) % 4, 1, 3, ym).wait_send()


def gather(counts, tokens, out_grad, tiles):
    return pl.pallas_call(
        gather_kernel,
        name="gather",
        out_shape=(
            pltpu.VMEM((8 * ROWS, WIDTH), BF),
            pltpu.VMEM((8 * ROWS, WIDTH), BF),
            pltpu.VMEM((SLOTS, 32, 4, TILE), BF),
        ),
        in_specs=[SM, ANY, ANY, VM],
        out_specs=(ANY, ANY, ANY),
        scratch_shapes=[
            pltpu.VMEM((SLOTS, 4, TILE), BF),
            pltpu.SemaphoreType.DMA((2, 8, 3)),
            pltpu.SemaphoreType.DMA((2, 8)),
            pltpu.SemaphoreType.DMA((32, 7)),
            pltpu.SemaphoreType.DMA((32, 2)),
            pltpu.SemaphoreType.DMA((3,)),
        ],
        compiler_params=pltpu.CompilerParams(
            collective_id=0, has_side_effects=True, vmem_limit_bytes=4 * 1024 * 1024
        ),
    )(counts, tokens, out_grad, tiles)


def dot(a, b, dims):
    return lax.dot_general(a, b, (dims, ((), ())), preferred_element_type=F32)


def block_kernel(scale, counts, rows, x, g, w, f_out, i_out, tg, acc_f, acc_i):
    acc_f[...] = jnp.zeros_like(acc_f)
    acc_i[...] = jnp.zeros_like(acc_i)

    def column(ref, r):
        return ref.at[:, pl.ds(pl.multiple_of(r * TILE, TILE), TILE)]

    def step(j, offsets):
        tiles, blocks, live, where = [], [], [], []
        for m in range(3):
            n = counts[m, j]
            src = x if m < 2 else g
            tiles.append([])
            blocks.append([])
            live.append([])
            where.append([])
            for k in range(3):
                on = k < n
                r = rows[m, k, j]
                at = m * CAP + offsets[m] + k
                tile = w[jnp.minimum(at, SLOTS - 1)]
                if k:
                    tile = jnp.where(on, tile, jnp.zeros_like(tile))
                tiles[m].append(tile)
                blocks[m].append(column(src, r)[...])
                live[m].append(on)
                where[m].append((r, at))
        x0 = jnp.concatenate(blocks[0], axis=1)
        x1 = jnp.concatenate(blocks[1], axis=1)
        g2 = jnp.concatenate(blocks[2], axis=1)
        w0 = jnp.concatenate(tiles[0], axis=0)
        w1 = jnp.concatenate(tiles[1], axis=0)
        w2 = jnp.concatenate(tiles[2], axis=1)
        gate = dot(x0, w0, ((1,), (0,)))
        up = dot(x1, w1, ((1,), (0,)))
        dh = dot(g2, w2, ((1,), (1,)))
        sig = jax.nn.sigmoid(gate)
        act = gate * sig
        hidden = (act * up).astype(BF)
        d_gate = (dh * up * sig * (1.0 + gate * (1.0 - sig))).astype(BF)
        d_up = (dh * act).astype(BF)
        for m, (value, acc) in enumerate(((d_gate, acc_i), (d_up, acc_i), (hidden, acc_f))):
            wide = dot(value, (w0, w1, w2)[m], ((1,), (1 if m < 2 else 0,)))
            if m < 2:
                terms = dot((x0, x1)[m], value, ((0,), (0,))) * scale
            else:
                terms = dot(value, g2, ((0,), (0,))) * scale
            for k in range(3):
                r, at = where[m][k]

                def put():
                    column(acc, r)[...] += wide[:, k * TILE : (k + 1) * TILE]
                    part = (
                        terms[k * TILE : (k + 1) * TILE]
                        if m < 2
                        else terms[:, k * TILE : (k + 1) * TILE]
                    )
                    tg[at] = part.astype(BF)

                if k:
                    pl.when(live[m][k])(put)
                else:
                    put()
        return tuple(offsets[m] + counts[m, j] for m in range(3))

    lax.fori_loop(0, BLOCKS, step, (jnp.int32(0),) * 3)
    f_out[...] = acc_f[...].astype(BF)
    i_out[...] = acc_i[...].astype(BF)


def compute(counts, rows, x, g, w, scale):
    return pl.pallas_call(
        functools.partial(block_kernel, scale),
        name="blocks",
        out_shape=(
            pltpu.VMEM(x.shape, BF),
            pltpu.VMEM(x.shape, BF),
            pltpu.VMEM((SLOTS, TILE, TILE), BF),
        ),
        in_specs=[SM, SM, VM, VM, VM],
        out_specs=(VM, VM, VM),
        scratch_shapes=[pltpu.VMEM(x.shape, F32), pltpu.VMEM(x.shape, F32)],
        compiler_params=pltpu.CompilerParams(vmem_limit_bytes=32 * 1024 * 1024),
    )(counts, rows, x, g, w)


def scatter_kernel(
    f_in,
    i_in,
    tg,
    f_out,
    i_out,
    w_out,
    own,
    mate_in,
    from_left,
    from_right,
    total,
    tx0,
    tx1,
    tx2,
    xa,
    xb,
    xs_lo,
    xs_hi,
    xl,
    xr,
    yb,
    ya,
    yc,
    ys_lo,
    ys_hi,
    yl,
    yr,
    z_own,
    z_send,
    z_in,
    act_local,
    act_mate_s,
    act_mate_r,
    act_send,
    act_left,
    act_right,
    x_local,
    x_send,
    x_recv,
    y_send,
    y_recv,
    z_sems,
):
    zh, x, y, z, c = places()
    t = z * 2 + c
    ins, outs = (f_in, i_in), (f_out, i_out)
    greet(zh, x, y, z, c)
    lo, hi = pl.ds(0, HALF), pl.ds(HALF, HALF)
    xp, xm = piece_at(zh, (x + 1) % 4, y), piece_at(zh, (x + 3) % 4, y)
    yp, ym = piece_at(zh, x, (y + 1) % 4), piece_at(zh, x, (y + 3) % 4)
    zo = piece_at(1 - zh, x, y)

    def remote(src, dst, send, recv, peer):
        return pltpu.make_async_remote_copy(
            src_ref=src,
            dst_ref=dst,
            send_sem=send,
            recv_sem=recv,
            device_id=peer,
            device_id_type=MESH,
        )

    def rows_of(arr, shard):
        return ins[arr].at[pl.ds(pl.multiple_of(shard * ROWS, ROWS), ROWS)]

    def mate_copy(arr, zz):
        return remote(
            rows_of(arr, zz * 2 + 1 - c),
            mate_in.at[arr, zz],
            act_mate_s.at[arr, zz],
            act_mate_r.at[arr, zz],
            {"tensor": z * 2 + 1 - c},
        )

    def own_copy(arr, zz):
        return pltpu.make_async_copy(
            rows_of(arr, zz * 2 + c), own.at[arr, zz], act_local.at[arr, zz]
        )

    def tx_copy(n):
        return pltpu.make_async_copy(tg.at[:, :, (x + (3, 1, 0)[n]) % 4], (tx0, tx1, tx2)[n], x_local.at[n])

    px, mx = {"dp": xp}, {"dp": xm}
    opp, fwd, bwd = (x + 2) % 4, (x + 1) % 4, (x + 3) % 4
    x_copies = [
        remote(tg.at[lo, :, opp], xa, x_send.at[0], x_recv.at[0], px),
        remote(tg.at[hi, :, opp], xb, x_send.at[1], x_recv.at[1], mx),
        remote(tg.at[hi, :, fwd], xl.at[hi], x_send.at[2], x_recv.at[2], px),
        remote(tg.at[lo, :, bwd], xr.at[lo], x_send.at[3], x_recv.at[3], mx),
        remote(xs_lo, xl.at[lo], x_send.at[4], x_recv.at[4], px),
        remote(xs_hi, xr.at[hi], x_send.at[5], x_recv.at[5], mx),
    ]
    for n in range(4):
        x_copies[n].start()
    order = ((0, 3), (0, 0), (1, 3), (1, 0), (0, 2), (0, 1), (1, 2), (1, 1))
    for arr, zz in order:
        mate_copy(arr, zz).start()
        own_copy(arr, zz).start()
    for n in range(3):
        tx_copy(n).start()

    def along(arr, zz, buf, sems, way, first):
        own_copy(arr, zz).wait()
        mate_copy(arr, zz).wait_recv()
        hop = remote(
            total.at[arr, zz], buf.at[arr, zz], act_send.at[arr, zz], sems.at[arr, zz],
            {"tensor": t + way},
        )
        if first:
            chunks(total, (own, mate_in), arr, zz)
        else:
            hop.wait_recv()
            chunks(total, (own, mate_in, buf), arr, zz)
        hop.start()

    def chunks(dst, srcs, *lead):
        for n in range(0, WIDTH, 512):
            s = pl.ds(n, 512)
            at = (*lead, slice(None), s)
            acc = srcs[0][at].astype(F32)
            for src in srcs[1:]:
                acc = acc + src[at].astype(F32)
            if dst is total:
                dst[at] = acc.astype(BF)
            else:
                dst[:, s] = acc.astype(BF)

    def ends():
        @pl.when(z == 0)
        def _():
            for zz in (3, 2, 1):
                for arr in range(2):
                    along(arr, zz, from_left, act_left, 2, True)

        @pl.when(z == 3)
        def _():
            for zz in (0, 1, 2):
                for arr in range(2):
                    along(arr, zz, from_right, act_right, -2, True)

    def middle(arr, n):
        @pl.when(z == 1)
        def _():
            if n < 2:
                along(arr, 3 - n, from_left, act_left, 2, False)
            else:
                along(arr, 0, from_right, act_right, -2, False)

        @pl.when(z == 2)
        def _():
            if n < 2:
                along(arr, n, from_right, act_right, -2, False)
            else:
                along(arr, 3, from_left, act_left, 2, False)

    def final(arr):
        own_copy(arr, z).wait()
        mate_copy(arr, z).wait_recv()

        @pl.when(z > 0)
        def _():
            remote(
                total.at[arr, z], from_left.at[arr, z], act_send.at[arr, z], act_left.at[arr, z],
                {"tensor": t},
            ).wait_recv()

        @pl.when(z < 3)
        def _():
            remote(
                total.at[arr, z], from_right.at[arr, z], act_send.at[arr, z], act_right.at[arr, z],
                {"tensor": t},
            ).wait_recv()

        base = (own, mate_in)
        for has_left, has_right in ((False, True), (True, True), (True, False)):
            here = (z == 0) if not has_left else ((z == 3) if not has_right else (z > 0) & (z < 3))
            bufs = base + ((from_left,) if has_left else ()) + ((from_right,) if has_right else ())

            @pl.when(here)
            def _():
                chunks(outs[arr], bufs, arr, z)

    def each(n, body):
        def step(i, _):
            body(i)
            return 0

        lax.fori_loop(0, n, step, 0)

    ends()
    middle(0, 0)

    tx_copy(1).wait()
    x_copies[0].wait_recv()

    def add_lo(i):
        for h in range(2):
            xs_lo[i, h] = (tx1[i, h].astype(F32) + xa[i, h].astype(F32)).astype(BF)

    each(HALF, add_lo)
    x_copies[4].start()
    tx_copy(0).wait()
    x_copies[1].wait_recv()

    def add_hi(i):
        for h in range(2):
            xs_hi[i, h] = (tx0[HALF + i, h].astype(F32) + xb[i, h].astype(F32)).astype(BF)

    each(HALF, add_hi)
    x_copies[5].start()
    middle(1, 0)
    middle(0, 2)
    middle(0, 1)
    middle(1, 2)

    tx_copy(2).wait()
    for n in (2, 3, 4, 5):
        x_copies[n].wait_recv()

    def x_final(i):
        for h in range(2):
            v = tx2[i, h].astype(F32) + xl[i, h].astype(F32) + xr[i, h].astype(F32)
            for q in range(4):
                yb[q, i, h] = v[4 * q : 4 * q + 4].astype(BF)

    each(SLOTS, x_final)
    py, my = {"dp": yp}, {"dp": ym}
    yo, yf, yw = (y + 2) % 4, (y + 1) % 4, (y + 3) % 4
    y_copies = [
        remote(yb.at[yo, lo], ya, y_send.at[0], y_recv.at[0], py),
        remote(yb.at[yo, hi], yc, y_send.at[1], y_recv.at[1], my),
        remote(yb.at[yf, hi], yl.at[hi], y_send.at[2], y_recv.at[2], py),
        remote(yb.at[yw, lo], yr.at[lo], y_send.at[3], y_recv.at[3], my),
        remote(ys_lo, yl.at[lo], y_send.at[4], y_recv.at[4], py),
        remote(ys_hi, yr.at[hi], y_send.at[5], y_recv.at[5], my),
    ]
    for n in range(4):
        y_copies[n].start()
    middle(1, 1)
    y_copies[0].wait_recv()

    def add_ylo(i):
        ys_lo[i] = (yb[yf, i].astype(F32) + ya[i].astype(F32)).astype(BF)

    each(HALF, add_ylo)
    y_copies[4].start()
    y_copies[1].wait_recv()

    def add_yhi(i):
        ys_hi[i] = (yb[yw, HALF + i].astype(F32) + yc[i].astype(F32)).astype(BF)

    each(HALF, add_yhi)
    y_copies[5].start()
    for n in (2, 3, 4, 5):
        y_copies[n].wait_recv()

    def y_final(i):
        def of(h):
            return yb[y, i, h].astype(F32) + yl[i, h].astype(F32) + yr[i, h].astype(F32)

        z_own[i] = of(zh)
        z_send[i] = of(1 - zh).astype(BF)

    each(SLOTS, y_final)
    z_copy = remote(z_send, z_in, z_sems.at[0], z_sems.at[1], {"dp": zo})
    z_copy.start()
    final(0)
    final(1)
    z_copy.wait_recv()

    def z_final(i):
        w_out[i] = (z_own[i] + z_in[i].astype(F32)).astype(BF)

    each(SLOTS, z_final)
    for arr in range(2):
        for zz in range(4):
            mate_copy(arr, zz).wait_send()

            @pl.when(z != zz)
            def _():
                remote(
                    total.at[arr, zz],
                    from_left.at[arr, zz],
                    act_send.at[arr, zz],
                    act_left.at[arr, zz],
                    {"tensor": t},
                ).wait_send()

    for copy in x_copies + y_copies + [z_copy]:
        copy.wait_send()


def scatter(f, i, tg):
    act = pltpu.VMEM((2, 4, ROWS, WIDTH), BF)
    dma = pltpu.SemaphoreType.DMA
    return pl.pallas_call(
        scatter_kernel,
        name="scatter",
        out_shape=(
            jax.ShapeDtypeStruct((ROWS, WIDTH), BF),
            jax.ShapeDtypeStruct((ROWS, WIDTH), BF),
            jax.ShapeDtypeStruct((SLOTS, 4, TILE), BF),
        ),
        in_specs=[ANY, ANY, ANY],
        out_specs=(VM, VM, VM),
        scratch_shapes=[act] * 5
        + [pltpu.VMEM((SLOTS, 2, 16, TILE), BF)] * 3
        + [pltpu.VMEM((HALF, 2, 16, TILE), BF)] * 4
        + [pltpu.VMEM((SLOTS, 2, 16, TILE), BF)] * 2
        + [pltpu.VMEM((4, SLOTS, 2, 4, TILE), BF)]
        + [pltpu.VMEM((HALF, 2, 4, TILE), BF)] * 4
        + [pltpu.VMEM((SLOTS, 2, 4, TILE), BF)] * 2
        + [pltpu.VMEM((SLOTS, 4, TILE), F32)]
        + [pltpu.VMEM((SLOTS, 4, TILE), BF)] * 2
        + [dma((2, 4))] * 6
        + [dma((3,)), dma((6,)), dma((6,)), dma((6,)), dma((6,)), dma((2,))],
        compiler_params=pltpu.CompilerParams(
            collective_id=1, has_side_effects=True, vmem_limit_bytes=36 * 1024 * 1024
        ),
    )(f, i, tg)


def finish_kernel(counts, f_in, i_in, w_in, f_out, i_out, w_out):
    f_out[...] = f_in[...]
    i_out[...] = i_in[...]
    for m in range(3):

        def expand(j, base):
            n = counts[m, j]
            for k in range(3):
                v = w_in[jnp.minimum(base + k, SLOTS - 1)]
                w_out[m * 42 + j * 3 + k] = jnp.where(k < n, v, jnp.zeros_like(v))
            return base + n

        lax.fori_loop(0, BLOCKS, expand, jnp.int32(m * CAP))


def finish(counts, f, i, tg):
    return pl.pallas_call(
        finish_kernel,
        name="finish",
        out_shape=(
            jax.ShapeDtypeStruct(f.shape, BF),
            jax.ShapeDtypeStruct(i.shape, BF),
            jax.ShapeDtypeStruct((3 * 42, 4, TILE), BF),
        ),
        in_specs=[SM, VM, VM, VM],
        out_specs=(VM, VM, VM),
        compiler_params=pltpu.CompilerParams(vmem_limit_bytes=4 * 1024 * 1024),
    )(counts, f, i, tg)


def shards(tokens, out_grad, weight_tiles, tile_counts, tile_rows):
    scale = 1.0 / math.sqrt(8192)
    tiles = weight_tiles.transpose(1, 2, 3, 0, 4).reshape(126, 4, TILE)
    rows = tile_rows.transpose(0, 2, 1)
    tokens, out_grad, tiles, tile_counts, rows = (
        pltpu.with_memory_space_constraint(v, pltpu.HBM)
        for v in (tokens, out_grad, tiles, tile_counts, rows)
    )
    x, g, w = gather(tile_counts, tokens, out_grad, tiles)
    f, i, tg = compute(tile_counts, rows, x, g, w.reshape(SLOTS, TILE, TILE), scale)
    f, i, tg = scatter(f, i, tg.reshape(SLOTS, 2, 4, 16, TILE))
    f, i, tg = finish(tile_counts, f, i, tg)
    tile_grad = tg.reshape(3, BLOCKS, 3, 4, TILE).transpose(3, 0, 1, 2, 4)
    return (f, i, tile_grad)


def solution(mesh):
    return jax.shard_map(
        shards,
        mesh=mesh,
        in_specs=(
            P(("dp", "tensor"), None),
            P(("dp", "tensor"), None),
            P("dp", None, "tensor", None, None),
            P(None, "tensor"),
            P(None, "tensor", None),
        ),
        out_specs=(
            P(("dp", "tensor"), None),
            P(("dp", "tensor"), None),
            P("dp", None, "tensor", None, None),
        ),
        check_vma=False,
    )
```

```python
import functools
import math

import jax
import jax.numpy as jnp
from jax import lax
from jax.experimental import pallas as pl
from jax.experimental.pallas import tpu as pltpu
from jax.sharding import PartitionSpec as P

MESH = pl.DeviceIdType.MESH
BF = jnp.bfloat16
F32 = jnp.float32
ANY = pl.BlockSpec(memory_space=pl.ANY)
VM = pl.BlockSpec(memory_space=pltpu.VMEM)
SM = pl.BlockSpec(memory_space=pltpu.SMEM)

CAP = 28
SLOTS = 3 * CAP
HALF = SLOTS // 2
BLOCKS = 14
ROWS = 32
WIDTH = 4096
TILE = 128


def places():
    d = lax.axis_index("dp")
    t = lax.axis_index("tensor")
    return d // 16, (d // 4) % 4, d % 4, t // 2, t % 2


def piece_at(zh, x, y):
    return zh * 16 + x * 4 + y


def greet(zh, x, y, z, c):
    barrier = pltpu.get_barrier_semaphore()
    peers = [
        {"tensor": ((z + 1) % 4) * 2 + c},
        {"tensor": ((z + 3) % 4) * 2 + c},
        {"tensor": z * 2 + 1 - c},
        {"dp": piece_at(zh, x, (y + 1) % 4)},
        {"dp": piece_at(zh, x, (y + 3) % 4)},
        {"dp": piece_at(zh, (x + 1) % 4, y)},
        {"dp": piece_at(zh, (x + 3) % 4, y)},
        {"dp": piece_at(1 - zh, x, y)},
    ]
    for peer in peers:
        pl.semaphore_signal(barrier, inc=1, device_id=peer, device_id_type=MESH)
    pl.semaphore_wait(barrier, len(peers))


def gather_kernel(
    counts, x_in, g_in, w_in, x_out, g_out, w_out, w_own, xs_send, xs_recv, w_send, w_recv, local
):
    zh, x, y, z, c = places()
    t = z * 2 + c
    ins, outs = (x_in, g_in), (x_out, g_out)
    greet(zh, x, y, z, c)

    def rows_of(arr, shard):
        return outs[arr].at[pl.ds(pl.multiple_of(shard * ROWS, ROWS), ROWS)]

    def act_copy(arr, shard, way, src, peer):
        return pltpu.make_async_remote_copy(
            src_ref=src,
            dst_ref=rows_of(arr, shard),
            send_sem=xs_send.at[arr, shard, way],
            recv_sem=xs_recv.at[arr, shard],
            device_id={"tensor": peer},
            device_id_type=MESH,
        )

    right, left, mate = t + 2, t - 2, z * 2 + 1 - c

    def to(arr, shard, way, src):
        return act_copy(arr, shard, way, src, (right, left, mate)[way])

    def compact(m):
        def step(i, carry):
            j, k = carry
            w_own[m * CAP + i] = w_in[m * 42 + j * 3 + k]
            more = k + 1 < counts[m, j]
            return (
                jnp.where(more, j, jnp.minimum(j + 1, BLOCKS - 1)),
                jnp.where(more, k + 1, 0),
            )

        lax.fori_loop(0, CAP, step, (jnp.int32(0), jnp.int32(0)))

    for m in range(3):
        compact(m)

    me = piece_at(zh, x, y)
    halves = (pl.ds(0, HALF), pl.ds(HALF, HALF))

    def w_part(piece, half):
        if half is None:
            return w_out.at[:, piece]
        return w_out.at[halves[half], piece]

    def w_copy(piece, half, way, peer, src=None):
        return pltpu.make_async_remote_copy(
            src_ref=w_part(piece, half) if src is None else src,
            dst_ref=w_part(piece, half),
            send_sem=w_send.at[piece, way],
            recv_sem=w_recv.at[piece, 1 if half == 1 else 0],
            device_id={"dp": peer},
            device_id_type=MESH,
        )

    xp, xm = piece_at(zh, (x + 1) % 4, y), piece_at(zh, (x + 3) % 4, y)
    yp, ym = piece_at(zh, x, (y + 1) % 4), piece_at(zh, x, (y + 3) % 4)
    zo = piece_at(1 - zh, x, y)

    w_copy(me, None, 6, zo, w_own).start()
    w_copy(me, None, 2, yp, w_own).start()
    w_copy(me, None, 3, ym, w_own).start()
    w_copy(me, None, 0, xp, w_own).start()
    w_copy(me, None, 1, xm, w_own).start()
    for arr in range(2):

        @pl.when(z < 3)
        def _():
            to(arr, t, 0, ins[arr]).start()

        @pl.when(z > 0)
        def _():
            to(arr, t, 1, ins[arr]).start()

        to(arr, t, 2, ins[arr]).start()
    own_copies = [
        pltpu.make_async_copy(x_in, rows_of(0, t), local.at[0]),
        pltpu.make_async_copy(g_in, rows_of(1, t), local.at[1]),
        pltpu.make_async_copy(w_own, w_out.at[:, me], local.at[2]),
    ]
    for copy in own_copies:
        copy.start()

    def along_y(h):
        base = h * 16 + x * 4
        near, far, opp = base + (y + 3) % 4, base + (y + 1) % 4, base + (y + 2) % 4
        w_copy(near, None, 0, me).wait_recv()
        w_copy(near, 0, 2, yp).start()
        w_copy(near, None, 0, xp).start()
        w_copy(near, None, 1, xm).start()
        w_copy(far, None, 0, me).wait_recv()
        w_copy(far, 1, 3, ym).start()
        w_copy(far, None, 0, xp).start()
        w_copy(far, None, 1, xm).start()
        w_copy(opp, 0, 0, me).wait_recv()
        w_copy(opp, 1, 0, me).wait_recv()
        w_copy(opp, None, 0, xp).start()
        w_copy(opp, None, 1, xm).start()

    def along_x(h):
        for dy in (0, 3, 1, 2):
            yy = (y + dy) % 4
            near = h * 16 + ((x + 3) % 4) * 4 + yy
            far = h * 16 + ((x + 1) % 4) * 4 + yy
            w_copy(near, None, 0, me).wait_recv()
            w_copy(near, 0, 4, xp).start()
            w_copy(far, None, 0, me).wait_recv()
            w_copy(far, 1, 5, xm).start()

    def along_z(n, arr):
        @pl.when(z - n >= 0)
        def _():
            shard = t - 2 * n
            act_copy(arr, shard, 0, rows_of(arr, shard), t).wait_recv()

            @pl.when(z < 3)
            def _():
                to(arr, shard, 0, rows_of(arr, shard)).start()

            to(arr, shard, 2, rows_of(arr, shard)).start()

        @pl.when(z + n <= 3)
        def _():
            shard = t + 2 * n
            act_copy(arr, shard, 0, rows_of(arr, shard), t).wait_recv()

            @pl.when(z > 0)
            def _():
                to(arr, shard, 1, rows_of(arr, shard)).start()

            to(arr, shard, 2, rows_of(arr, shard)).start()

    along_y(zh)
    zpiece = zo
    w_copy(zpiece, None, 0, me).wait_recv()
    w_copy(zpiece, None, 2, yp).start()
    w_copy(zpiece, None, 3, ym).start()
    w_copy(zpiece, None, 0, xp).start()
    w_copy(zpiece, None, 1, xm).start()
    along_z(1, 0)
    along_y(1 - zh)
    along_z(1, 1)
    along_x(zh)
    along_z(2, 0)
    along_x(1 - zh)
    along_z(2, 1)
    along_z(3, 0)
    along_z(3, 1)

    for zz in range(4):
        for arr in range(2):
            act_copy(arr, zz * 2 + 1 - c, 0, rows_of(arr, zz * 2 + 1 - c), t).wait_recv()
    for h in range(2):
        for yy in range(4):
            opp = h * 16 + ((x + 2) % 4) * 4 + yy
            w_copy(opp, 0, 0, me).wait_recv()
            w_copy(opp, 1, 0, me).wait_recv()
    for copy in own_copies:
        copy.wait()

    for arr in range(2):
        for zz in range(4):
            shard = zz * 2 + c

            @pl.when((zz <= z) & (z < 3))
            def _():
                to(arr, shard, 0, ins[arr]).wait_send()

            @pl.when((zz >= z) & (z > 0))
            def _():
                to(arr, shard, 1, ins[arr]).wait_send()

            to(arr, shard, 2, ins[arr]).wait_send()
    w_copy(me, None, 6, zo, w_own).wait_send()
    for h in range(2):
        base = h * 16 + x * 4
        for dy in range(4):
            yy = (y + dy) % 4
            w_copy(base + yy, None, 0, xp).wait_send()
            w_copy(base + yy, None, 1, xm).wait_send()
            w_copy(h * 16 + ((x + 3) % 4) * 4 + yy, 0, 4, xp).wait_send()
            w_copy(h * 16 + ((x + 1) % 4) * 4 + yy, 1, 5, xm).wait_send()
        w_copy(base + y, None, 2, yp).wait_send()
        w_copy(base + y, None, 3, ym).wait_send()
        w_copy(base + (y + 3) % 4, 0, 2, yp).wait_send()
        w_copy(base + (y + 1) % 4, 1, 3, ym).wait_send()


def gather(counts, tokens, out_grad, tiles):
    return pl.pallas_call(
        gather_kernel,
        name="gather",
        out_shape=(
            pltpu.VMEM((8 * ROWS, WIDTH), BF),
            pltpu.VMEM((8 * ROWS, WIDTH), BF),
            pltpu.VMEM((SLOTS, 32, 4, TILE), BF),
        ),
        in_specs=[SM, ANY, ANY, VM],
        out_specs=(ANY, ANY, ANY),
        scratch_shapes=[
            pltpu.VMEM((SLOTS, 4, TILE), BF),
            pltpu.SemaphoreType.DMA((2, 8, 3)),
            pltpu.SemaphoreType.DMA((2, 8)),
            pltpu.SemaphoreType.DMA((32, 7)),
            pltpu.SemaphoreType.DMA((32, 2)),
            pltpu.SemaphoreType.DMA((3,)),
        ],
        compiler_params=pltpu.CompilerParams(
            collective_id=0, has_side_effects=True, vmem_limit_bytes=4 * 1024 * 1024
        ),
    )(counts, tokens, out_grad, tiles)


def dot(a, b, dims):
    return lax.dot_general(a, b, (dims, ((), ())), preferred_element_type=F32)


def block_kernel(scale, counts, rows, x, g, w, f_out, i_out, tg, acc_f, acc_i):
    acc_f[...] = jnp.zeros_like(acc_f)
    acc_i[...] = jnp.zeros_like(acc_i)

    def column(ref, r):
        return ref.at[:, pl.ds(pl.multiple_of(r * TILE, TILE), TILE)]

    def step(j, offsets):
        tiles, blocks, live, where = [], [], [], []
        for m in range(3):
            n = counts[m, j]
            src = x if m < 2 else g
            tiles.append([])
            blocks.append([])
            live.append([])
            where.append([])
            for k in range(3):
                on = k < n
                r = rows[m, k, j]
                at = m * CAP + offsets[m] + k
                tile = w[jnp.minimum(at, SLOTS - 1)]
                if k:
                    tile = jnp.where(on, tile, jnp.zeros_like(tile))
                tiles[m].append(tile)
                blocks[m].append(column(src, r)[...])
                live[m].append(on)
                where[m].append((r, at))
        x0 = jnp.concatenate(blocks[0], axis=1)
        x1 = jnp.concatenate(blocks[1], axis=1)
        g2 = jnp.concatenate(blocks[2], axis=1)
        w0 = jnp.concatenate(tiles[0], axis=0)
        w1 = jnp.concatenate(tiles[1], axis=0)
        w2 = jnp.concatenate(tiles[2], axis=1)
        gate = dot(x0, w0, ((1,), (0,)))
        up = dot(x1, w1, ((1,), (0,)))
        dh = dot(g2, w2, ((1,), (1,)))
        sig = jax.nn.sigmoid(gate)
        act = gate * sig
        hidden = (act * up).astype(BF)
        d_gate = (dh * up * sig * (1.0 + gate * (1.0 - sig))).astype(BF)
        d_up = (dh * act).astype(BF)
        for m, (value, acc) in enumerate(((d_gate, acc_i), (d_up, acc_i), (hidden, acc_f))):
            wide = dot(value, (w0, w1, w2)[m], ((1,), (1 if m < 2 else 0,)))
            if m < 2:
                terms = dot((x0, x1)[m], value, ((0,), (0,))) * scale
            else:
                terms = dot(value, g2, ((0,), (0,))) * scale
            for k in range(3):
                r, at = where[m][k]

                column(acc, r)[...] += wide[:, k * TILE : (k + 1) * TILE]
                part = (
                    terms[k * TILE : (k + 1) * TILE]
                    if m < 2
                    else terms[:, k * TILE : (k + 1) * TILE]
                )
                tg[jnp.where(live[m][k], at, SLOTS) if k else at] = part.astype(BF)
        return tuple(offsets[m] + counts[m, j] for m in range(3))

    lax.fori_loop(0, BLOCKS, step, (jnp.int32(0),) * 3, unroll=2)
    f_out[...] = acc_f[...].astype(BF)
    i_out[...] = acc_i[...].astype(BF)


def compute(counts, rows, x, g, w, scale):
    return pl.pallas_call(
        functools.partial(block_kernel, scale),
        name="blocks",
        out_shape=(
            pltpu.VMEM(x.shape, BF),
            pltpu.VMEM(x.shape, BF),
            pltpu.VMEM((SLOTS + 1, TILE, TILE), BF),
        ),
        in_specs=[SM, SM, VM, VM, VM],
        out_specs=(VM, VM, VM),
        scratch_shapes=[pltpu.VMEM(x.shape, F32), pltpu.VMEM(x.shape, F32)],
        compiler_params=pltpu.CompilerParams(vmem_limit_bytes=32 * 1024 * 1024),
    )(counts, rows, x, g, w)


def scatter_kernel(
    f_in,
    i_in,
    tg,
    f_out,
    i_out,
    w_out,
    own,
    mate_in,
    from_left,
    from_right,
    total,
    tx0,
    tx1,
    tx2,
    xa,
    xb,
    xs_lo,
    xs_hi,
    xl,
    xr,
    yb,
    ya,
    yc,
    ys_lo,
    ys_hi,
    yl,
    yr,
    z_own,
    z_send,
    z_in,
    act_local,
    act_mate_s,
    act_mate_r,
    act_send,
    act_left,
    act_right,
    x_local,
    x_send,
    x_recv,
    y_send,
    y_recv,
    z_sems,
):
    zh, x, y, z, c = places()
    t = z * 2 + c
    ins, outs = (f_in, i_in), (f_out, i_out)
    greet(zh, x, y, z, c)
    lo, hi = pl.ds(0, HALF), pl.ds(HALF, HALF)
    xp, xm = piece_at(zh, (x + 1) % 4, y), piece_at(zh, (x + 3) % 4, y)
    yp, ym = piece_at(zh, x, (y + 1) % 4), piece_at(zh, x, (y + 3) % 4)
    zo = piece_at(1 - zh, x, y)

    def remote(src, dst, send, recv, peer):
        return pltpu.make_async_remote_copy(
            src_ref=src,
            dst_ref=dst,
            send_sem=send,
            recv_sem=recv,
            device_id=peer,
            device_id_type=MESH,
        )

    def rows_of(arr, shard):
        return ins[arr].at[pl.ds(pl.multiple_of(shard * ROWS, ROWS), ROWS)]

    def mate_copy(arr, zz):
        return remote(
            rows_of(arr, zz * 2 + 1 - c),
            mate_in.at[arr, zz],
            act_mate_s.at[arr, zz],
            act_mate_r.at[arr, zz],
            {"tensor": z * 2 + 1 - c},
        )

    def own_copy(arr, zz):
        return pltpu.make_async_copy(
            rows_of(arr, zz * 2 + c), own.at[arr, zz], act_local.at[arr, zz]
        )

    def tx_copy(n):
        return pltpu.make_async_copy(tg.at[pl.ds(0, SLOTS), :, (x + (3, 1, 0)[n]) % 4], (tx0, tx1, tx2)[n], x_local.at[n])

    px, mx = {"dp": xp}, {"dp": xm}
    opp, fwd, bwd = (x + 2) % 4, (x + 1) % 4, (x + 3) % 4
    x_copies = [
        remote(tg.at[lo, :, opp], xa, x_send.at[0], x_recv.at[0], px),
        remote(tg.at[hi, :, opp], xb, x_send.at[1], x_recv.at[1], mx),
        remote(tg.at[hi, :, fwd], xl.at[hi], x_send.at[2], x_recv.at[2], px),
        remote(tg.at[lo, :, bwd], xr.at[lo], x_send.at[3], x_recv.at[3], mx),
        remote(xs_lo, xl.at[lo], x_send.at[4], x_recv.at[4], px),
        remote(xs_hi, xr.at[hi], x_send.at[5], x_recv.at[5], mx),
    ]
    for n in range(4):
        x_copies[n].start()
    order = ((0, 3), (0, 0), (1, 3), (1, 0), (0, 2), (0, 1), (1, 2), (1, 1))
    for arr, zz in order:
        mate_copy(arr, zz).start()
        own_copy(arr, zz).start()
    for n in range(3):
        tx_copy(n).start()

    def along(arr, zz, buf, sems, way, first):
        own_copy(arr, zz).wait()
        mate_copy(arr, zz).wait_recv()
        hop = remote(
            total.at[arr, zz], buf.at[arr, zz], act_send.at[arr, zz], sems.at[arr, zz],
            {"tensor": t + way},
        )
        if first:
            chunks(total, (own, mate_in), arr, zz)
        else:
            hop.wait_recv()
            chunks(total, (own, mate_in, buf), arr, zz)
        hop.start()

    def chunks(dst, srcs, *lead):
        for n in range(0, WIDTH, 512):
            s = pl.ds(n, 512)
            at = (*lead, slice(None), s)
            acc = srcs[0][at].astype(F32)
            for src in srcs[1:]:
                acc = acc + src[at].astype(F32)
            if dst is total:
                dst[at] = acc.astype(BF)
            else:
                dst[:, s] = acc.astype(BF)

    def ends():
        @pl.when(z == 0)
        def _():
            for zz in (3, 2, 1):
                for arr in range(2):
                    along(arr, zz, from_left, act_left, 2, True)

        @pl.when(z == 3)
        def _():
            for zz in (0, 1, 2):
                for arr in range(2):
                    along(arr, zz, from_right, act_right, -2, True)

    def middle(arr, n):
        @pl.when(z == 1)
        def _():
            if n < 2:
                along(arr, 3 - n, from_left, act_left, 2, False)
            else:
                along(arr, 0, from_right, act_right, -2, False)

        @pl.when(z == 2)
        def _():
            if n < 2:
                along(arr, n, from_right, act_right, -2, False)
            else:
                along(arr, 3, from_left, act_left, 2, False)

    def final(arr):
        own_copy(arr, z).wait()
        mate_copy(arr, z).wait_recv()

        @pl.when(z > 0)
        def _():
            remote(
                total.at[arr, z], from_left.at[arr, z], act_send.at[arr, z], act_left.at[arr, z],
                {"tensor": t},
            ).wait_recv()

        @pl.when(z < 3)
        def _():
            remote(
                total.at[arr, z], from_right.at[arr, z], act_send.at[arr, z], act_right.at[arr, z],
                {"tensor": t},
            ).wait_recv()

        base = (own, mate_in)
        for has_left, has_right in ((False, True), (True, True), (True, False)):
            here = (z == 0) if not has_left else ((z == 3) if not has_right else (z > 0) & (z < 3))
            bufs = base + ((from_left,) if has_left else ()) + ((from_right,) if has_right else ())

            @pl.when(here)
            def _():
                chunks(outs[arr], bufs, arr, z)

    def each(n, body):
        def step(i, _):
            body(i)
            return 0

        lax.fori_loop(0, n, step, 0)

    ends()
    middle(0, 0)

    tx_copy(1).wait()
    x_copies[0].wait_recv()

    def add_lo(i):
        for h in range(2):
            xs_lo[i, h] = (tx1[i, h].astype(F32) + xa[i, h].astype(F32)).astype(BF)

    each(HALF, add_lo)
    x_copies[4].start()
    tx_copy(0).wait()
    x_copies[1].wait_recv()

    def add_hi(i):
        for h in range(2):
            xs_hi[i, h] = (tx0[HALF + i, h].astype(F32) + xb[i, h].astype(F32)).astype(BF)

    each(HALF, add_hi)
    x_copies[5].start()
    middle(1, 0)
    middle(0, 2)
    middle(0, 1)
    middle(1, 2)

    tx_copy(2).wait()
    for n in (2, 3, 4, 5):
        x_copies[n].wait_recv()

    def x_final(i):
        for h in range(2):
            v = tx2[i, h].astype(F32) + xl[i, h].astype(F32) + xr[i, h].astype(F32)
            for q in range(4):
                yb[q, i, h] = v[4 * q : 4 * q + 4].astype(BF)

    each(SLOTS, x_final)
    py, my = {"dp": yp}, {"dp": ym}
    yo, yf, yw = (y + 2) % 4, (y + 1) % 4, (y + 3) % 4
    y_copies = [
        remote(yb.at[yo, lo], ya, y_send.at[0], y_recv.at[0], py),
        remote(yb.at[yo, hi], yc, y_send.at[1], y_recv.at[1], my),
        remote(yb.at[yf, hi], yl.at[hi], y_send.at[2], y_recv.at[2], py),
        remote(yb.at[yw, lo], yr.at[lo], y_send.at[3], y_recv.at[3], my),
        remote(ys_lo, yl.at[lo], y_send.at[4], y_recv.at[4], py),
        remote(ys_hi, yr.at[hi], y_send.at[5], y_recv.at[5], my),
    ]
    for n in range(4):
        y_copies[n].start()
    middle(1, 1)
    y_copies[0].wait_recv()

    def add_ylo(i):
        ys_lo[i] = (yb[yf, i].astype(F32) + ya[i].astype(F32)).astype(BF)

    each(HALF, add_ylo)
    y_copies[4].start()
    y_copies[1].wait_recv()

    def add_yhi(i):
        ys_hi[i] = (yb[yw, HALF + i].astype(F32) + yc[i].astype(F32)).astype(BF)

    each(HALF, add_yhi)
    y_copies[5].start()
    for n in (2, 3, 4, 5):
        y_copies[n].wait_recv()

    def y_final(i):
        def of(h):
            return yb[y, i, h].astype(F32) + yl[i, h].astype(F32) + yr[i, h].astype(F32)

        z_own[i] = of(zh)
        z_send[i] = of(1 - zh).astype(BF)

    each(SLOTS, y_final)
    z_copy = remote(z_send, z_in, z_sems.at[0], z_sems.at[1], {"dp": zo})
    z_copy.start()
    final(0)
    final(1)
    z_copy.wait_recv()

    def z_final(i):
        w_out[i] = (z_own[i] + z_in[i].astype(F32)).astype(BF)

    each(SLOTS, z_final)
    for arr in range(2):
        for zz in range(4):
            mate_copy(arr, zz).wait_send()

            @pl.when(z != zz)
            def _():
                remote(
                    total.at[arr, zz],
                    from_left.at[arr, zz],
                    act_send.at[arr, zz],
                    act_left.at[arr, zz],
                    {"tensor": t},
                ).wait_send()

    for copy in x_copies + y_copies + [z_copy]:
        copy.wait_send()


def scatter(f, i, tg):
    act = pltpu.VMEM((2, 4, ROWS, WIDTH), BF)
    dma = pltpu.SemaphoreType.DMA
    return pl.pallas_call(
        scatter_kernel,
        name="scatter",
        out_shape=(
            jax.ShapeDtypeStruct((ROWS, WIDTH), BF),
            jax.ShapeDtypeStruct((ROWS, WIDTH), BF),
            jax.ShapeDtypeStruct((SLOTS, 4, TILE), BF),
        ),
        in_specs=[ANY, ANY, ANY],
        out_specs=(VM, VM, VM),
        scratch_shapes=[act] * 5
        + [pltpu.VMEM((SLOTS, 2, 16, TILE), BF)] * 3
        + [pltpu.VMEM((HALF, 2, 16, TILE), BF)] * 4
        + [pltpu.VMEM((SLOTS, 2, 16, TILE), BF)] * 2
        + [pltpu.VMEM((4, SLOTS, 2, 4, TILE), BF)]
        + [pltpu.VMEM((HALF, 2, 4, TILE), BF)] * 4
        + [pltpu.VMEM((SLOTS, 2, 4, TILE), BF)] * 2
        + [pltpu.VMEM((SLOTS, 4, TILE), F32)]
        + [pltpu.VMEM((SLOTS, 4, TILE), BF)] * 2
        + [dma((2, 4))] * 6
        + [dma((3,)), dma((6,)), dma((6,)), dma((6,)), dma((6,)), dma((2,))],
        compiler_params=pltpu.CompilerParams(
            collective_id=1, has_side_effects=True, vmem_limit_bytes=36 * 1024 * 1024
        ),
    )(f, i, tg)


def finish_kernel(counts, f_in, i_in, w_in, f_out, i_out, w_out):
    f_out[...] = f_in[...]
    i_out[...] = i_in[...]
    for m in range(3):

        def expand(j, base):
            n = counts[m, j]
            for k in range(3):
                v = w_in[jnp.minimum(base + k, SLOTS - 1)]
                w_out[m * 42 + j * 3 + k] = jnp.where(k < n, v, jnp.zeros_like(v))
            return base + n

        lax.fori_loop(0, BLOCKS, expand, jnp.int32(m * CAP))


def finish(counts, f, i, tg):
    return pl.pallas_call(
        finish_kernel,
        name="finish",
        out_shape=(
            jax.ShapeDtypeStruct(f.shape, BF),
            jax.ShapeDtypeStruct(i.shape, BF),
            jax.ShapeDtypeStruct((3 * 42, 4, TILE), BF),
        ),
        in_specs=[SM, VM, VM, VM],
        out_specs=(VM, VM, VM),
        compiler_params=pltpu.CompilerParams(vmem_limit_bytes=4 * 1024 * 1024),
    )(counts, f, i, tg)


def shards(tokens, out_grad, weight_tiles, tile_counts, tile_rows):
    scale = 1.0 / math.sqrt(8192)
    tiles = weight_tiles.transpose(1, 2, 3, 0, 4).reshape(126, 4, TILE)
    rows = tile_rows.transpose(0, 2, 1)
    tokens, out_grad, tiles, tile_counts, rows = (
        pltpu.with_memory_space_constraint(v, pltpu.HBM)
        for v in (tokens, out_grad, tiles, tile_counts, rows)
    )
    x, g, w = gather(tile_counts, tokens, out_grad, tiles)
    f, i, tg = compute(tile_counts, rows, x, g, w.reshape(SLOTS, TILE, TILE), scale)
    f, i, tg = scatter(f, i, tg.reshape(SLOTS + 1, 2, 4, 16, TILE))
    f, i, tg = finish(tile_counts, f, i, tg)
    tile_grad = tg.reshape(3, BLOCKS, 3, 4, TILE).transpose(3, 0, 1, 2, 4)
    return (f, i, tile_grad)


def solution(mesh):
    return jax.shard_map(
        shards,
        mesh=mesh,
        in_specs=(
            P(("dp", "tensor"), None),
            P(("dp", "tensor"), None),
            P("dp", None, "tensor", None, None),
            P(None, "tensor"),
            P(None, "tensor", None),
        ),
        out_specs=(
            P(("dp", "tensor"), None),
            P(("dp", "tensor"), None),
            P("dp", None, "tensor", None, None),
        ),
        check_vma=False,
    )
```
